32 devices in a mesh: samples: 8 (over z, y), variants: 4 (over x, core).
Axes of the slice: x: 2, y: 2, z: 4, core: 2. Of those that a mesh axis runs over, the one named last changes fastest.
Arguments:
- genotypes: int32 [2048, 32768], P('variants', 'samples'), may hold values from 0 to 3, as said below
- weights: float32 [32768], P('samples'), may hold values from 0.25 to 20
Outputs:
- call_mean: float32 [2048], P('variants')
- call_var: float32 [2048], P('variants')
- class_counts: int32 [4, 2048], P(None, 'variants')
- ld_window: float32 [1024, 2048], P('samples', 'variants')
- sample_calls: int32 [2, 32768], P(None, 'samples')
- sample_share: float32 [32768], P('samples')
The draws below stay inside these ranges and needn't reach their ends.
Inputs may be any that keep to these rules, and one draw needn't show every extreme that they name: `genotypes`: in every variant's row, each aligned group of 8 samples (samples 8 i to 8 i + 7) holds at least one call other than 3.
All inputs are finite; a program needn't handle non-finite values.
Results may differ from the reference program's by a relative error of at most 0.0004.
Values may be sent and summed in bfloat16 or wider, within the bound.
A program may use at most 64 MiB of HBM per device.

```python
import jax
import jax.numpy as jnp
from jax import lax

VAR_DEV = 512
VARIANTS = 2048
SAMPLES = 32768


def draw_genotypes(key, part):
    keys = jax.random.split(key, 6)
    level_all = jax.random.randint(keys[0], (VARIANTS,), 150, 500)
    hold_all = jax.random.randint(keys[1], (VARIANTS,), 300, 850)
    gap_all = jax.random.randint(keys[2], (VARIANTS,), 20, 400)
    step_keys = jax.random.split(keys[3], VARIANTS)
    slot = jnp.arange(SAMPLES, dtype=jnp.int32) % 8
    first_start = jax.random.randint(keys[4], (SAMPLES,), 0, 1000) < 300
    second_start = jax.random.randint(keys[5], (SAMPLES,), 0, 1000) < 300

    def advance(carry, inputs):
        first_hap, second_hap = carry
        step_key, level, hold, gap = inputs
        pieces = jax.random.split(step_key, 6)
        fresh_one = jax.random.randint(pieces[0], (SAMPLES,), 0, 1000) < level
        fresh_two = jax.random.randint(pieces[1], (SAMPLES,), 0, 1000) < level
        keep_one = jax.random.randint(pieces[2], (SAMPLES,), 0, 1000) < hold
        keep_two = jax.random.randint(pieces[3], (SAMPLES,), 0, 1000) < hold
        new_one = jnp.where(keep_one, first_hap, fresh_one)
        new_two = jnp.where(keep_two, second_hap, fresh_two)
        chosen = jnp.repeat(jax.random.randint(pieces[5], (SAMPLES // 8,), 0, 8), 8)
        lost = (jax.random.randint(pieces[4], (SAMPLES,), 0, 1000) < gap) & (slot != chosen)
        calls = jnp.where(lost, 3, new_one.astype(jnp.int32) + new_two.astype(jnp.int32))
        return ((new_one, new_two), calls.astype(jnp.int32))
    final_state, rows = lax.scan(advance, (first_start, second_start), (step_keys, level_all, hold_all, gap_all))
    return rows


def draw_weights(key, part):
    position = jnp.arange(SAMPLES, dtype=jnp.float32) / max(SAMPLES - 1, 1)
    base = jnp.exp(jax.random.uniform(key, (SAMPLES,), jnp.float32, jnp.log(0.3), jnp.log(3.0)))
    rise = 1.0 + 2.0 * position
    return (base * rise).astype(jnp.float32)


def setup_inputs(seed: int = 0) -> dict:
    key_list = jax.random.split(jax.random.key(seed), 3)
    genotypes = draw_genotypes(jax.random.fold_in(key_list[2], 71), 0)
    weights = draw_weights(jax.random.fold_in(key_list[2], 71), 0)
    return dict(genotypes=genotypes, weights=weights)


def reference(genotypes, weights):
    block_count = VARIANTS // VAR_DEV
    blocks = genotypes.reshape(block_count, VAR_DEV, SAMPLES)
    root_weight = jnp.sqrt(weights)

    def block_stats(block):
        present = block != 3
        called = present.astype(jnp.float32)
        dosage = jnp.where(present, block, 0).astype(jnp.float32)
        weighted = called * weights[None, :]
        w_sum = lax.optimization_barrier(jnp.sum(weighted, axis=1))
        mean_value = lax.optimization_barrier(jnp.sum(weighted * dosage, axis=1)) / w_sum
        centered = (dosage - mean_value[:, None]) * called
        var_value = lax.optimization_barrier(jnp.sum(weighted * centered * centered, axis=1)) / w_sum
        counts = jnp.stack([lax.optimization_barrier(jnp.sum((block == level).astype(jnp.int32), axis=1)) for level in range(4)])
        factor = 1.0 / jnp.sqrt(w_sum * (var_value + 1e-05))
        scaled = (root_weight[None, :] * centered * factor[:, None]).astype(jnp.bfloat16)
        return (mean_value, var_value, counts, scaled)
    mean_value, var_value, counts, scaled = lax.map(block_stats, blocks)
    padded = jnp.concatenate([scaled, jnp.zeros((1, VAR_DEV, SAMPLES), scaled.dtype)], axis=0)

    def window(index):
        own = lax.dynamic_index_in_dim(padded, index, 0, keepdims=False)
        after = lax.dynamic_index_in_dim(padded, index + 1, 0, keepdims=False)
        joined = jnp.concatenate([own, after], axis=0).astype(jnp.float32)
        return jnp.dot(joined, own.astype(jnp.float32).T, preferred_element_type=jnp.float32)
    ld_blocks = lax.map(window, jnp.arange(block_count, dtype=jnp.int32))
    ld_window = ld_blocks.transpose(1, 0, 2).reshape(2 * VAR_DEV, VARIANTS)

    def sample_block(block_pair):
        block, scaled_block = block_pair
        squares = scaled_block.astype(jnp.float32)
        return (lax.optimization_barrier(jnp.sum((block != 3).astype(jnp.int32), axis=0)), lax.optimization_barrier(jnp.sum((block == 1).astype(jnp.int32), axis=0)), lax.optimization_barrier(jnp.sum(squares * squares, axis=0)))
    called_rows, het_rows, square_rows = lax.map(sample_block, (blocks, scaled))
    sample_calls = jnp.stack([lax.optimization_barrier(jnp.sum(called_rows, axis=0)), lax.optimization_barrier(jnp.sum(het_rows, axis=0))])
    sample_share = lax.optimization_barrier(jnp.sum(square_rows, axis=0)) * (SAMPLES / VARIANTS)
    return (mean_value.reshape(VARIANTS), var_value.reshape(VARIANTS), counts.transpose(1, 0, 2).reshape(4, VARIANTS), ld_window, sample_calls, sample_share)
```

```python
import functools

import jax
import jax.numpy as jnp
from jax import lax
from jax.experimental import pallas as pl
from jax.experimental.pallas import tpu as pltpu
from jax.sharding import PartitionSpec as P

MESH = pl.DeviceIdType.MESH
F32 = jnp.float32
BF16 = jnp.bfloat16
LANES = 128
STEP = 16
SUB = 32
FULL = 32400.0
SLAB = 512
EARLY = 7
LEFT = 16


def aligned(x, n):
    return pl.multiple_of(x, n)


def kernel(
    S,
    V,
    gen_hbm,
    w_ref,
    stat_out,
    count_out,
    ld_out,
    call_out,
    share_out,
    gen,
    code,
    ncode,
    pcode,
    scaled,
    other,
    keep_o,
    keep_x,
    ypart_o,
    yrcv_o,
    ypart_n,
    yrcv_n,
    ypart_p,
    yrcv_p,
    zpart_o,
    zpart_n,
    zpart_p,
    zrcv,
    zrcv_p,
    wacc,
    cacc,
    sacc,
    qacc,
    root,
    gat,
    par,
    npar,
    ppar,
    aux,
    col_o,
    col_x,
    lane_o,
    lane_x,
    lane_q,
    tall,
    spread,
    smp_mine,
    smp_mate,
    smp_all,
    gen_sem,
    ncode_send,
    ncode_recv,
    pcode_send,
    pcode_recv,
    stat_send,
    stat_recv,
    par_send,
    par_recv,
    yo_send,
    yo_recv,
    yn_send,
    yn_recv,
    yp_send,
    yp_recv,
    zo_send,
    zn_send,
    zp_send,
    z_recv,
    zp_recv,
    mate_send,
    mate_recv,
    smp_send,
    smp_recv,
):
    s = lax.axis_index("samples")
    v = lax.axis_index("variants")
    rows, width = gen.shape
    R = 2 * rows // S
    H = S // 2
    Q = H // 2
    PAIRS = S // 2
    NP = rows // SUB
    UNIT = min(R, 64)
    NCP = rows // LANES
    KL = width * LEFT // 32 // LANES * LANES
    C = V // 2
    blocks = width // LANES
    slabs = width // SLAB

    pair = lax.div(s, 2)
    y = s - 2 * pair
    mate = s + 1 - 2 * y
    chip = lax.div(v, 2)
    odd = v - 2 * chip == 1
    even = jnp.logical_not(odd)
    near = 2 * chip < C
    far = jnp.logical_not(near)
    has_next = v < V - 1
    has_prev = v > 0
    next_part = jnp.logical_and(odd, has_next)
    next_full = jnp.logical_and(even, near)
    prev_part = jnp.logical_and(even, has_prev)
    prev_full = jnp.logical_and(odd, far)
    send_down_full = jnp.logical_and(odd, near)
    send_down_part = prev_part
    send_up_full = jnp.logical_and(even, far)
    send_up_part = next_part
    from_next = jnp.logical_or(next_part, next_full)
    from_prev = jnp.logical_or(send_up_full, send_up_part)
    does_prev = jnp.logical_or(prev_part, prev_full)
    down = lax.rem(v + V - 1, V)
    up = lax.rem(v + 1, V)
    turn = lax.div(lax.div(pair * NP, PAIRS), 4) * 4

    def piece_rows(i):
        return pl.ds(aligned(lax.rem(i + turn, NP) * SUB, SUB), SUB)

    def load(i):
        return pltpu.make_async_copy(
            gen_hbm.at[piece_rows(i)], gen.at[piece_rows(i)], gen_sem.at[i]
        )

    def loop(start, stop, body):
        def step(i, _):
            body(i)
            return 0

        lax.fori_loop(start, stop, step, 0)

    loop(0, NP, lambda i: load(i).start())

    barrier = pltpu.get_barrier_semaphore()

    def greet(device):
        pl.semaphore_signal(barrier, inc=1, device_id=device, device_id_type=MESH)

    loop(1, S, lambda d: greet({"samples": lax.rem(s + d, S)}))
    loop(1, V, lambda d: greet({"variants": lax.rem(v + d, V)}))

    def cross_greet(d):
        there = 2 * lax.rem(pair + d, PAIRS) + y

        @pl.when(has_prev)
        def _():
            greet({"samples": there, "variants": down})

        @pl.when(has_next)
        def _():
            greet({"samples": there, "variants": up})

    loop(1, PAIRS, cross_greet)
    greetings = (
        S
        + V
        - 2
        + (PAIRS - 1) * (has_prev.astype(jnp.int32) + has_next.astype(jnp.int32))
    )

    root[...] = jnp.sqrt(w_ref[...])
    sacc[...] = jnp.zeros_like(sacc)
    qacc[...] = jnp.zeros_like(qacc)

    def piece_copy(i, buf, send, recv, device, lo, hi):
        here = piece_rows(i)
        return pltpu.make_async_remote_copy(
            src_ref=code.at[here, lo:hi],
            dst_ref=buf.at[here, lo:hi],
            send_sem=send.at[i],
            recv_sem=recv.at[i],
            device_id={"variants": device},
            device_id_type=MESH,
        )

    def down_copy(i, hi):
        return piece_copy(i, ncode, ncode_send, ncode_recv, down, 0, hi)

    def up_copy(i, lo):
        return piece_copy(i, pcode, pcode_send, pcode_recv, up, lo, width)

    def send_far(i):
        @pl.when(send_down_part)
        def _():
            down_copy(i, KL).start()

        @pl.when(send_up_part)
        def _():
            up_copy(i, KL).start()

    def first_pass(k):
        load(k).wait()
        base = lax.rem(k + turn, NP) * SUB

        def sixteen(i):
            here = pl.ds(aligned(base + i * STEP, STEP), STEP)
            zero = jnp.zeros((STEP, LANES), F32)
            w0, w1, w2 = zero, zero, zero
            cnt = jnp.zeros((STEP, LANES), jnp.int32)
            for b in range(blocks):
                lane = slice(b * LANES, (b + 1) * LANES)
                g = gen[here, lane]
                w = jnp.broadcast_to(w_ref[0:1, lane], (STEP, LANES))
                w0 = w0 + jnp.where(g == 0, w, 0.0)
                w1 = w1 + jnp.where(g == 1, w, 0.0)
                w2 = w2 + jnp.where(g == 2, w, 0.0)
                tag = jnp.left_shift(jnp.int32(1), jnp.left_shift(g, 3))
                cnt = cnt + tag
                sacc[:, lane] += tag[:8] + tag[8:]
                code[here, lane] = g.astype(F32).astype(BF16)
            wacc[0, here] = w0
            wacc[1, here] = w1
            wacc[2, here] = w2
            cacc[here] = cnt

        loop(0, SUB // STEP, sixteen)

        @pl.when(k == 0)
        def _():
            pl.semaphore_wait(barrier, greetings)

        @pl.when(send_down_full)
        def _():
            down_copy(k, width).start()

        @pl.when(send_up_full)
        def _():
            up_copy(k, 0).start()

        @pl.when(k < EARLY)
        def _():
            send_far(k)

    loop(0, NP, first_pass)

    def total(x):
        return jnp.sum(x.T, axis=0, keepdims=True)

    cnt = cacc[...]
    lines = [total(wacc[i]) for i in range(3)]
    for level in range(4):
        lines.append(
            total(jnp.bitwise_and(jnp.right_shift(cnt, 8 * level), 255).astype(F32))
        )
    lines.append(jnp.zeros_like(lines[0]))
    gat[s] = jnp.concatenate(lines, axis=0)

    def stat_copy(d, slot):
        return pltpu.make_async_remote_copy(
            src_ref=gat.at[slot],
            dst_ref=gat.at[slot],
            send_sem=stat_send.at[d],
            recv_sem=stat_recv.at[slot],
            device_id={"samples": lax.rem(s + d, S)},
            device_id_type=MESH,
        )

    loop(1, S, lambda d: stat_copy(d, s).start())
    loop(1, S, lambda d: stat_copy(d, lax.rem(s + d, S)).wait_recv())

    sums = gat[0]
    for t in range(1, S):
        sums = sums + gat[t]
    w0, w1, w2 = sums[0:1], sums[1:2], sums[2:3]
    w_sum = w0 + w1 + w2
    mean = (w1 + 2.0 * w2) / w_sum
    one, two = 1.0 - mean, 2.0 - mean
    ms, os, ts = mean * mean, one * one, two * two
    var = (w0 * ms + w1 * os + w2 * ts) / w_sum
    factor = 1.0 / jnp.sqrt(w_sum * (var + 1e-05))
    par[0:1] = mean
    par[1:2] = factor
    for t in range(S):
        length = jnp.sqrt(gat[t, 0:1] * ms + gat[t, 1:2] * os + gat[t, 2:3] * ts)
        par[2 + t : 3 + t] = jnp.maximum(length * factor, 1e-12)
    spare = par.shape[0] - 2 - S
    if spare:
        par[2 + S :] = jnp.zeros((spare, rows), F32)

    def par_copy(i, dst, device):
        return pltpu.make_async_remote_copy(
            src_ref=par,
            dst_ref=dst,
            send_sem=par_send.at[i],
            recv_sem=par_recv.at[i],
            device_id={"variants": device},
            device_id_type=MESH,
        )

    @pl.when(has_prev)
    def _():
        par_copy(0, npar, down).start()

    @pl.when(from_prev)
    def _():
        par_copy(1, ppar, up).start()

    loop(EARLY, NP, send_far)

    stat_out[...] = jnp.concatenate([mean, var], axis=0)
    count_out[...] = sums[3:7].astype(jnp.int32)

    def build(src, col, lane):
        def of(who):
            line = jnp.zeros((1, rows), F32)
            for t in range(S):
                line = line + src[2 + t : 3 + t] * (who == t).astype(F32)
            return line

        mine, its = of(s), of(mate)
        both = jnp.sqrt(mine * mine + its * its)
        aux[...] = jnp.concatenate(
            [src[0:2], FULL / mine, its, FULL / both, jnp.zeros((3, rows), F32)],
            axis=0,
        )
        turned = aux[...].T
        for i in range(5):
            col[i] = jnp.broadcast_to(turned[:, i : i + 1], (rows, LANES))
        lane[0:1] = 1.0 / mine
        lane[1:2] = its * (1.0 / FULL)
        lane[2:3] = 1.0 / both
        sizes = []
        for q in range(PAIRS):
            a, b = src[2 + 2 * q : 3 + 2 * q], src[3 + 2 * q : 4 + 2 * q]
            sizes.append(jnp.sqrt(a * a + b * b))
        left = -PAIRS % 8
        if left:
            sizes.append(jnp.zeros((left, rows), F32))
        tall[:, 0 : PAIRS + left] = jnp.concatenate(sizes, axis=0).T

    def scale(src, src_row, dst, dst_row, count, lo, hi, col, squares):
        def sixteen(i):
            here = pl.ds(aligned(src_row + i * STEP, STEP), STEP)
            there = pl.ds(aligned(dst_row + i * STEP, STEP), STEP)
            m, f = col[0, here], col[1, here]
            for b in range(lo // LANES, hi // LANES):
                lane = slice(b * LANES, (b + 1) * LANES)
                d = src[here, lane].astype(F32)
                r = jnp.broadcast_to(root[0:1, lane], (STEP, LANES))
                x = jnp.where(d < 2.5, r * (d - m) * f, 0.0).astype(BF16)
                dst[there, lane] = x
                if squares:
                    yy = x.astype(F32)
                    yy = yy * yy
                    qacc[:, lane] += yy[:8] + yy[8:]

        loop(0, count // STEP, sixteen)

    def rows_of():
        row = lax.rem(s, H) * R
        for q in range(PAIRS):
            spread[q] = jnp.broadcast_to(
                tall[pl.ds(aligned(row, R), R), q : q + 1], (R, LANES)
            )

    build(par, col_o, lane_o)
    for q in range(PAIRS):
        lane_q[q] = jnp.sqrt(
            par[2 + 2 * q : 3 + 2 * q] ** 2 + par[3 + 2 * q : 4 + 2 * q] ** 2
        ) * (1.0 / FULL)

    @pl.when(s < H)
    def _():
        rows_of()

    scale(code, 0, scaled, 0, rows, 0, width, col_o, True)

    def dot(a, b):
        return lax.dot_general(
            a, b, (((1,), (1,)), ((), ())), preferred_element_type=F32
        )

    def coded(value, e, line):
        q = jnp.round(value * e * line)
        q = jnp.clip(q, -32767.0, 32767.0)
        return q.astype(jnp.int32).astype(jnp.int16)

    def pack(src, src_row, col, col_row, lane, lane_at, cols, count, dst, dst_row):
        def sixteen(i):
            here = pl.ds(aligned(src_row + i * STEP, STEP), STEP)
            e = col[2, pl.ds(aligned(col_row + i * STEP, STEP), STEP)]
            for b in range(cols // LANES):
                part = slice(b * LANES, (b + 1) * LANES)
                line = lane[0:1, pl.ds(aligned(lane_at + b * LANES, LANES), LANES)]
                dst[pl.ds(aligned(dst_row + i * STEP, STEP), STEP), part] = coded(
                    src[here, part], e, line
                )

        loop(0, count // STEP, sixteen)

    def merge(
        src,
        src_row,
        got,
        got_row,
        col,
        col_row,
        lane,
        lane_at,
        cols,
        count,
        dst,
        dst_row,
        final,
    ):
        def sixteen(i):
            here = pl.ds(aligned(src_row + i * STEP, STEP), STEP)
            line_rows = pl.ds(aligned(col_row + i * STEP, STEP), STEP)
            there = pl.ds(aligned(dst_row + i * STEP, STEP), STEP)
            theirs = pl.ds(aligned(got_row + i * STEP, STEP), STEP)
            d, e = col[3, line_rows], col[4, line_rows]
            for b in range(cols // LANES):
                part = slice(b * LANES, (b + 1) * LANES)
                lanes = pl.ds(aligned(lane_at + b * LANES, LANES), LANES)
                q = got[theirs, part].astype(jnp.int32).astype(F32)
                value = src[here, part] + q * d * lane[1:2, lanes]
                if final:
                    dst[there, part] = value
                else:
                    dst[there, part] = coded(value, e, lane[2:3, lanes])

        loop(0, count // STEP, sixteen)

    def copy_to(src, dst, send, recv, device):
        return pltpu.make_async_remote_copy(
            src_ref=src,
            dst_ref=dst,
            send_sem=send,
            recv_sem=recv,
            device_id=device,
            device_id_type=MESH,
        )

    def yo_copy(j):
        return copy_to(
            ypart_o.at[j], yrcv_o.at[j], yo_send.at[j], yo_recv.at[j], {"samples": mate}
        )

    def zo_copy(j):
        return copy_to(
            zpart_o.at[j],
            zrcv.at[pair],
            zo_send.at[j],
            z_recv.at[pair],
            {"samples": 2 * j + y},
        )

    def own_dot(o):
        here = pl.ds(aligned(o * R, R), R)
        keep_o[here, :] = dot(scaled[here, :], scaled[...])

    def own_rows(k):
        give = k < Q
        j = lax.rem(lax.rem(k, Q) + pair, Q)
        o = 2 * j + jnp.where(give, 1 - y, y)
        own_dot(o)

        @pl.when(give)
        def _():
            pack(
                keep_o, o * R, col_o, o * R, lane_o, 0, rows, R, ypart_o.at[j], 0
            )
            yo_copy(j).start()

    loop(0, H, own_rows)

    packed = sacc[...]
    tags = [
        jnp.bitwise_and(jnp.right_shift(packed, 8 * level), 255).astype(F32)
        for level in range(3)
    ]
    for q, value in enumerate([tags[0] + tags[1] + tags[2], tags[1], qacc[...]]):
        line = jnp.sum(value, axis=0, keepdims=True)
        for i in range(slabs):
            at = q * slabs + i
            smp_mine[at : at + 1, :] = line[:, i * SLAB : (i + 1) * SLAB]

    mate_copy = copy_to(
        smp_mine,
        smp_mate,
        mate_send.at[0],
        mate_recv.at[0],
        {"variants": v + 1 - 2 * (v - 2 * chip)},
    )
    mate_copy.start()

    def collect_own(k):
        j = lax.rem(k + pair, Q)
        o = 2 * j + y
        yo_copy(j).wait_recv()
        args = (keep_o, o * R, yrcv_o.at[j], 0, col_o, o * R, lane_o, 0, rows, R)

        @pl.when(o == s)
        def _():
            merge(*args, ld_out, 0, True)

        @pl.when(o != s)
        def _():
            merge(*args, zpart_o.at[j], 0, False)
            zo_copy(j).start()

    def yn_copy(at, size):
        j = lax.div(lax.div(at, R), 2)
        here = pl.ds(aligned(at - lax.div(at, R) * R, size), size)
        unit = lax.div(at, UNIT)
        return copy_to(
            ypart_n.at[j, here],
            yrcv_n.at[j, here],
            yn_send.at[unit],
            yn_recv.at[unit],
            {"samples": mate},
        )

    def zn_copy(at, size):
        r = lax.div(at, R)
        here = pl.ds(aligned(at - r * R, size), size)
        return copy_to(
            zpart_n.at[lax.div(r, 2), here],
            zrcv.at[pair, here],
            zn_send.at[lax.div(at, UNIT)],
            z_recv.at[pair],
            {"samples": H + r},
        )

    def next_rows(k, size):
        return lax.rem(k * size + turn * SUB, rows)

    def next_parity(at):
        r = lax.div(at, R)
        return r - 2 * lax.div(r, 2) == y

    def collect_next(k, size):
        at = next_rows(k, size)
        r = lax.div(at, R)

        @pl.when(next_parity(at))
        def _():
            yn_copy(at, size).wait_recv()
            j = lax.div(r, 2)
            off = at - r * R
            args = (keep_x, at, yrcv_n.at[j], off, col_x, at, lane_o, 0, rows, size)

            @pl.when(H + r == s)
            def _():
                merge(*args, ld_out, off, True)

            @pl.when(H + r != s)
            def _():
                merge(*args, zpart_n.at[j], off, False)
                zn_copy(at, size).start()

    def next_role(size, hi):
        per = size // SUB

        def chunk(k):
            at = next_rows(k, size)
            for i in range(per):
                down_copy(k * per + i, hi).wait_recv()
            scale(ncode, at, other, 0, size, 0, hi, col_x, False)
            here = pl.ds(aligned(at, size), size)
            keep_x[here, :] = dot(other[0:size, 0:hi], scaled[:, 0:hi])
            r = lax.div(at, R)

            @pl.when(jnp.logical_not(next_parity(at)))
            def _():
                pack(
                    keep_x,
                    at,
                    col_x,
                    at,
                    lane_o,
                    0,
                    rows,
                    size,
                    ypart_n.at[lax.div(r, 2)],
                    at - r * R,
                )
                yn_copy(at, size).start()

            @pl.when(k > 0)
            def _():
                collect_next(k - 1, size)

        loop(0, rows // size, chunk)
        collect_next(rows // size - 1, size)

    def yp_copy(c):
        return copy_to(
            ypart_p.at[c], yrcv_p.at[c], yp_send.at[c], yp_recv.at[c], {"samples": mate}
        )

    def zp_copy(j, c):
        return copy_to(
            zpart_p.at[j, c],
            zrcv_p.at[pair, c],
            zp_send.at[j],
            zp_recv.at[pair],
            {"samples": H + 2 * j + y, "variants": down},
        )

    def prev_chunk(k):
        return lax.rem(k + lax.div(turn * SUB, LANES), NCP)

    def collect_prev(k):
        c = prev_chunk(k)
        yp_copy(c).wait_recv()

        def one(i):
            j = lax.rem(i + pair, Q)
            o = (2 * j + y) * R
            merge(
                keep_x,
                c * rows + o,
                yrcv_p.at[c, j],
                0,
                col_o,
                o,
                lane_x,
                c * LANES,
                LANES,
                R,
                zpart_p.at[j, c],
                0,
                False,
            )
            zp_copy(j, c).start()

        loop(0, Q, one)

    def prev_role(lo):
        per = LANES // SUB

        def chunk(k):
            c = prev_chunk(k)
            for i in range(per):
                up_copy(k * per + i, lo).wait_recv()
            scale(pcode, c * LANES, other, 0, LANES, lo, width, col_x, False)
            here = pl.ds(aligned(c * rows, rows), rows)
            keep_x[here, 0:LANES] = dot(scaled[:, lo:width], other[0:LANES, lo:width])

            def one(j):
                o = (2 * j + 1 - y) * R
                pack(
                    keep_x,
                    c * rows + o,
                    col_o,
                    o,
                    lane_x,
                    c * LANES,
                    LANES,
                    R,
                    ypart_p.at[c, j],
                    0,
                )

            loop(0, Q, one)
            yp_copy(c).start()

            @pl.when(k > 0)
            def _():
                collect_prev(k - 1)

        loop(0, NCP, chunk)
        collect_prev(NCP - 1)

    def with_next():
        par_copy(0, npar, down).wait_recv()
        build(npar, col_x, lane_x)

        @pl.when(s >= H)
        def _():
            rows_of()


    def with_prev():
        par_copy(1, ppar, up).wait_recv()
        build(ppar, col_x, lane_x)

    @pl.when(prev_full)
    def _():
        with_prev()
        prev_role(0)

    @pl.when(next_full)
    def _():
        with_next()
        next_role(R, width)

    loop(0, Q, collect_own)

    mate_copy.wait_recv()
    smp_all[chip] = smp_mine[...] + smp_mate[...]

    def smp_copy(d, slot):
        return copy_to(
            smp_all.at[slot],
            smp_all.at[slot],
            smp_send.at[d],
            smp_recv.at[slot],
            {"variants": lax.rem(v + 2 * d, V)},
        )

    loop(1, C, lambda d: smp_copy(d, chip).start())

    @pl.when(prev_part)
    def _():
        with_prev()
        prev_role(KL)

    @pl.when(next_part)
    def _():
        with_next()
        next_role(UNIT, KL)

    @pl.when(jnp.logical_and(jnp.logical_not(from_next), has_next))
    def _():
        with_next()

    loop(1, C, lambda d: smp_copy(d, lax.rem(chip + d, C)).wait_recv())
    all_sums = smp_all[0]
    for t in range(1, C):
        all_sums = all_sums + smp_all[t]
    call_out[...] = all_sums[: 2 * slabs].astype(jnp.int32)
    share_out[...] = all_sums[2 * slabs :] * F32((width * S) / (rows * V))

    def gather(got, q, part, wide):
        def sixteen(i):
            here = pl.ds(aligned(i * STEP, STEP), STEP)
            e = spread[q, here]
            for b in range(rows // LANES):
                lanes = slice(b * LANES, (b + 1) * LANES)
                line = lane_q[q, 0:1, lanes]
                piece = got[b, here] if wide else got[here, lanes]
                ld_out[here, lanes] += piece.astype(jnp.int32).astype(F32) * e * line

        loop(0, R // STEP, sixteen)

    def gather_pairs(d):
        q = lax.rem(pair + d, PAIRS)
        copy_to(
            zrcv.at[q], zrcv.at[q], zo_send.at[0], z_recv.at[q], {"samples": mate}
        ).wait_recv()
        gather(zrcv.at[q], q, None, False)

    def gather_prev(d):
        q = lax.rem(pair + d, PAIRS)
        copy_to(
            zrcv_p.at[q], zrcv_p.at[q], zp_send.at[0], zp_recv.at[q], {"samples": mate}
        ).wait_recv()
        gather(zrcv_p.at[q], q, None, True)

    @pl.when(s < H)
    def _():
        loop(1, PAIRS, gather_pairs)

    @pl.when(s >= H)
    def _():
        @pl.when(from_next)
        def _():
            loop(1, PAIRS, gather_pairs)

        @pl.when(jnp.logical_not(from_next))
        def _():
            ld_out[...] = jnp.zeros_like(ld_out)

        @pl.when(from_prev)
        def _():
            loop(0, PAIRS, gather_prev)

    loop(1, S, lambda d: stat_copy(d, s).wait_send())
    loop(1, C, lambda d: smp_copy(d, chip).wait_send())
    mate_copy.wait_send()

    def drain_own(j):
        yo_copy(j).wait_send()

        @pl.when(2 * j + y != s)
        def _():
            zo_copy(j).wait_send()

    loop(0, Q, drain_own)

    def drain_next(size):
        def one(k):
            at = next_rows(k, size)
            r = lax.div(at, R)
            mine = next_parity(at)

            @pl.when(jnp.logical_not(mine))
            def _():
                yn_copy(at, size).wait_send()

            @pl.when(jnp.logical_and(mine, H + r != s))
            def _():
                zn_copy(at, size).wait_send()

        loop(0, rows // size, one)

    @pl.when(next_full)
    def _():
        drain_next(R)

    @pl.when(next_part)
    def _():
        drain_next(UNIT)

    @pl.when(does_prev)
    def _():
        loop(0, NCP, lambda c: yp_copy(c).wait_send())

        def drain(j):
            copy_to(
                zpart_p.at[j], zpart_p.at[j], zp_send.at[j], zp_recv.at[0], {"samples": mate}
            ).wait_send()

        loop(0, Q, drain)

    @pl.when(has_prev)
    def _():
        par_copy(0, npar, down).wait_send()

    @pl.when(from_prev)
    def _():
        par_copy(1, ppar, up).wait_send()

    @pl.when(send_down_full)
    def _():
        loop(0, NP, lambda i: down_copy(i, width).wait_send())

    @pl.when(send_down_part)
    def _():
        loop(0, NP, lambda i: down_copy(i, KL).wait_send())

    @pl.when(send_up_full)
    def _():
        loop(0, NP, lambda i: up_copy(i, 0).wait_send())

    @pl.when(send_up_part)
    def _():
        loop(0, NP, lambda i: up_copy(i, KL).wait_send())


def finish(stats, counts, ld, calls, share, mean, var, counts_o, ld_o, calls_o, share_o):
    slabs = share.shape[0]
    mean[...] = stats[0]
    var[...] = stats[1]
    counts_o[...] = counts[...]
    ld_o[...] = ld[...]
    for i in range(slabs):
        here = slice(i * SLAB, (i + 1) * SLAB)
        for q in range(2):
            calls_o[q : q + 1, here] = calls[q * slabs + i : q * slabs + i + 1]
        share_o[here] = share[i]


def on_device(S, V, genotypes, weights):
    rows, width = genotypes.shape
    R = 2 * rows // S
    H = S // 2
    Q = H // 2
    PAIRS = S // 2
    C = V // 2
    NP = rows // SUB
    NCP = rows // LANES
    units = rows // min(R, 64)
    lines = -(-(2 + S) // 8) * 8
    slabs = width // SLAB
    vmem = pl.BlockSpec(memory_space=pltpu.VMEM)
    dma = pltpu.SemaphoreType.DMA
    stats, counts, ld, calls, share = pl.pallas_call(
        functools.partial(kernel, S, V),
        out_shape=(
            jax.ShapeDtypeStruct((2, rows), F32),
            jax.ShapeDtypeStruct((4, rows), jnp.int32),
            jax.ShapeDtypeStruct((R, rows), F32),
            jax.ShapeDtypeStruct((2 * slabs, SLAB), jnp.int32),
            jax.ShapeDtypeStruct((slabs, SLAB), F32),
        ),
        in_specs=[pl.BlockSpec(memory_space=pl.ANY), vmem],
        out_specs=(vmem,) * 5,
        scratch_shapes=[
            pltpu.VMEM((rows, width), jnp.int32),
            pltpu.VMEM((rows, width), BF16),
            pltpu.VMEM((rows, width), BF16),
            pltpu.VMEM((rows, width), BF16),
            pltpu.VMEM((rows, width), BF16),
            pltpu.VMEM((max(R, LANES), width), BF16),
            pltpu.VMEM((rows, rows), F32),
            pltpu.VMEM((NCP * rows, rows), F32),
            pltpu.VMEM((Q, R, rows), jnp.int16),
            pltpu.VMEM((Q, R, rows), jnp.int16),
            pltpu.VMEM((Q, R, rows), jnp.int16),
            pltpu.VMEM((Q, R, rows), jnp.int16),
            pltpu.VMEM((NCP, Q, R, LANES), jnp.int16),
            pltpu.VMEM((NCP, Q, R, LANES), jnp.int16),
            pltpu.VMEM((Q, R, rows), jnp.int16),
            pltpu.VMEM((Q, R, rows), jnp.int16),
            pltpu.VMEM((Q, NCP, R, LANES), jnp.int16),
            pltpu.VMEM((PAIRS, R, rows), jnp.int16),
            pltpu.VMEM((PAIRS, NCP, R, LANES), jnp.int16),
            pltpu.VMEM((3, rows, LANES), F32),
            pltpu.VMEM((rows, LANES), jnp.int32),
            pltpu.VMEM((8, width), jnp.int32),
            pltpu.VMEM((8, width), F32),
            pltpu.VMEM((1, width), F32),
            pltpu.VMEM((S, 8, rows), F32),
            pltpu.VMEM((lines, rows), F32),
            pltpu.VMEM((lines, rows), F32),
            pltpu.VMEM((lines, rows), F32),
            pltpu.VMEM((8, rows), F32),
            pltpu.VMEM((5, rows, LANES), F32),
            pltpu.VMEM((5, rows, LANES), F32),
            pltpu.VMEM((8, rows), F32),
            pltpu.VMEM((8, rows), F32),
            pltpu.VMEM((PAIRS, 1, rows), F32),
            pltpu.VMEM((rows, LANES), F32),
            pltpu.VMEM((PAIRS, R, LANES), F32),
            pltpu.VMEM((3 * slabs, SLAB), F32),
            pltpu.VMEM((3 * slabs, SLAB), F32),
            pltpu.VMEM((C, 3 * slabs, SLAB), F32),
            dma((NP,)),
            dma((NP,)),
            dma((NP,)),
            dma((NP,)),
            dma((NP,)),
            dma((S,)),
            dma((S,)),
            dma((2,)),
            dma((2,)),
            dma((Q,)),
            dma((Q,)),
            dma((units,)),
            dma((units,)),
            dma((NCP,)),
            dma((NCP,)),
            dma((Q,)),
            dma((units,)),
            dma((Q,)),
            dma((PAIRS,)),
            dma((PAIRS,)),
            dma((1,)),
            dma((1,)),
            dma((C,)),
            dma((C,)),
        ],
        compiler_params=pltpu.CompilerParams(
            collective_id=0, has_side_effects=True, vmem_limit_bytes=60 * 1024 * 1024
        ),
        name="window_stats",
    )(genotypes, weights.reshape(1, width))
    return pl.pallas_call(
        finish,
        out_shape=(
            jax.ShapeDtypeStruct((rows,), F32),
            jax.ShapeDtypeStruct((rows,), F32),
            jax.ShapeDtypeStruct((4, rows), jnp.int32),
            jax.ShapeDtypeStruct((R, rows), F32),
            jax.ShapeDtypeStruct((2, width), jnp.int32),
            jax.ShapeDtypeStruct((width,), F32),
        ),
        in_specs=[vmem] * 5,
        out_specs=(vmem,) * 6,
        name="finish",
    )(stats, counts, ld, calls, share)


def solution(mesh):
    body = functools.partial(on_device, mesh.shape["samples"], mesh.shape["variants"])
    return jax.shard_map(
        body,
        mesh=mesh,
        in_specs=(P("variants", "samples"), P("samples")),
        out_specs=(
            P("variants"),
            P("variants"),
            P(None, "variants"),
            P("samples", "variants"),
            P(None, "samples"),
            P("samples"),
        ),
        check_vma=False,
    )
```

```python
import functools

import jax
import jax.numpy as jnp
from jax import lax
from jax.experimental import pallas as pl
from jax.experimental.pallas import tpu as pltpu
from jax.sharding import PartitionSpec as P

MESH = pl.DeviceIdType.MESH
F32 = jnp.float32
BF16 = jnp.bfloat16
LANES = 128
STEP = 16
SUB = 32
FULL = 32400.0
SLAB = 512
EARLY = 7
LEFT = 16


def aligned(x, n):
    return pl.multiple_of(x, n)


def kernel(
    S,
    V,
    gen_hbm,
    w_hbm,
    stat_out,
    count_out,
    ld_out,
    call_out,
    share_out,
    gen,
    code,
    ncode,
    pcode,
    scaled,
    other,
    keep_o,
    keep_x,
    ypart_o,
    yrcv_o,
    ypart_n,
    yrcv_n,
    ypart_p,
    yrcv_p,
    zpart_o,
    zpart_n,
    zpart_p,
    zrcv,
    zrcv_p,
    wacc,
    cacc,
    sacc,
    qacc,
    root,
    gat,
    tally,
    par,
    npar,
    ppar,
    aux,
    col_o,
    col_x,
    lane_o,
    lane_x,
    lane_q,
    tall,
    spread,
    smp_mine,
    smp_mate,
    smp_all,
    w_ref,
    gen_sem,
    w_sem,
    ncode_send,
    ncode_recv,
    pcode_send,
    pcode_recv,
    stat_send,
    stat_recv,
    tally_send,
    tally_recv,
    par_send,
    par_recv,
    yo_send,
    yo_recv,
    yn_send,
    yn_recv,
    yp_send,
    yp_recv,
    zo_send,
    zn_send,
    zp_send,
    z_recv,
    zp_recv,
    mate_send,
    mate_recv,
    smp_send,
    smp_recv,
):
    s = lax.axis_index("samples")
    v = lax.axis_index("variants")
    rows, width = gen.shape
    R = 2 * rows // S
    H = S // 2
    Q = H // 2
    PAIRS = S // 2
    NP = rows // SUB
    GROUP = LANES // SUB
    UNIT = min(R, 64)
    NCP = rows // LANES
    KL = width * LEFT // 32 // LANES * LANES
    C = V // 2
    blocks = width // LANES
    slabs = width // SLAB

    pair = lax.div(s, 2)
    y = s - 2 * pair
    mate = s + 1 - 2 * y
    chip = lax.div(v, 2)
    odd = v - 2 * chip == 1
    even = jnp.logical_not(odd)
    near = 2 * chip < C
    far = jnp.logical_not(near)
    has_next = v < V - 1
    has_prev = v > 0
    next_part = jnp.logical_and(odd, has_next)
    next_full = jnp.logical_and(even, near)
    prev_part = jnp.logical_and(even, has_prev)
    prev_full = jnp.logical_and(odd, far)
    send_down_full = jnp.logical_and(odd, near)
    send_down_part = prev_part
    send_up_full = jnp.logical_and(even, far)
    send_up_part = next_part
    from_next = jnp.logical_or(next_part, next_full)
    from_prev = jnp.logical_or(send_up_full, send_up_part)
    does_prev = jnp.logical_or(prev_part, prev_full)
    does_full = jnp.logical_or(next_full, prev_full)
    hold = jnp.where(s == 0, 10, jnp.where(s < H, 5, 1))
    down = lax.rem(v + V - 1, V)
    up = lax.rem(v + 1, V)
    turn = lax.div(lax.div(pair * NP, PAIRS), 4) * 4

    def piece_rows(i):
        return pl.ds(aligned(lax.rem(i + turn, NP) * SUB, SUB), SUB)

    def load(i):
        return pltpu.make_async_copy(
            gen_hbm.at[piece_rows(i)], gen.at[piece_rows(i)], gen_sem.at[i]
        )

    def loop(start, stop, body):
        def step(i, _):
            body(i)
            return 0

        lax.fori_loop(start, stop, step, 0)

    w_load = pltpu.make_async_copy(w_hbm, w_ref, w_sem)
    load(0).start()
    w_load.start()
    loop(1, NP, lambda i: load(i).start())

    barrier = pltpu.get_barrier_semaphore()

    def greet(device):
        pl.semaphore_signal(barrier, inc=1, device_id=device, device_id_type=MESH)

    loop(1, S, lambda d: greet({"samples": lax.rem(s + d, S)}))
    loop(1, V, lambda d: greet({"variants": lax.rem(v + d, V)}))

    def cross_greet(d):
        there = 2 * lax.rem(pair + d, PAIRS) + y

        @pl.when(has_prev)
        def _():
            greet({"samples": there, "variants": down})

        @pl.when(has_next)
        def _():
            greet({"samples": there, "variants": up})

    loop(1, PAIRS, cross_greet)
    greetings = (
        S
        + V
        - 2
        + (PAIRS - 1) * (has_prev.astype(jnp.int32) + has_next.astype(jnp.int32))
    )

    sacc[...] = jnp.zeros_like(sacc)
    w_load.wait()
    root[...] = jnp.sqrt(w_ref[...])

    def piece_copy(i, buf, send, recv, device, lo, hi):
        here = piece_rows(i)
        return pltpu.make_async_remote_copy(
            src_ref=code.at[here, lo:hi],
            dst_ref=buf.at[here, lo:hi],
            send_sem=send.at[lax.rem(i + turn, NP)],
            recv_sem=recv.at[lax.rem(i + turn, NP)],
            device_id={"variants": device},
            device_id_type=MESH,
        )

    def down_copy(i, hi):
        return piece_copy(i, ncode, ncode_send, ncode_recv, down, 0, hi)

    def up_copy(i, lo):
        return piece_copy(i, pcode, pcode_send, pcode_recv, up, lo, width)

    def send_far(i):
        @pl.when(send_down_part)
        def _():
            down_copy(i, KL).start()

        @pl.when(send_up_part)
        def _():
            up_copy(i, KL).start()

    def total(x):
        return jnp.sum(x.T, axis=0, keepdims=True)

    def first_pass(k):
        load(k).wait()
        base = lax.rem(k + turn, NP) * SUB

        def sixteen(i):
            here = pl.ds(aligned(base + i * STEP, STEP), STEP)
            zero = jnp.zeros((STEP, LANES), F32)
            w0, w1, w2 = zero, zero, zero
            cnt = jnp.zeros((STEP, LANES), jnp.int32)
            for b in range(blocks):
                lane = slice(b * LANES, (b + 1) * LANES)
                g = gen[here, lane]
                w = jnp.broadcast_to(w_ref[0:1, lane], (STEP, LANES))
                w0 = w0 + jnp.where(g == 0, w, 0.0)
                w1 = w1 + jnp.where(g == 1, w, 0.0)
                w2 = w2 + jnp.where(g == 2, w, 0.0)
                tag = jnp.left_shift(jnp.int32(1), jnp.left_shift(g, 3))
                cnt = cnt + tag
                sacc[:, lane] += tag[:8] + tag[8:]
                code[here, lane] = g.astype(F32).astype(BF16)
            wacc[0, here] = w0
            wacc[1, here] = w1
            wacc[2, here] = w2
            cacc[here] = cnt

        loop(0, SUB // STEP, sixteen)

        @pl.when(lax.rem(k, GROUP) == GROUP - 1)
        def _():
            group = pl.ds(aligned(base + SUB - LANES, LANES), LANES)
            for i in range(3):
                gat[s, i : i + 1, group] = total(wacc[i, group])
            cnt = cacc[group]
            for level in range(4):
                some = jnp.bitwise_and(jnp.right_shift(cnt, 8 * level), 255)
                tally[s, level : level + 1, group] = total(some.astype(F32))

        def send(i):
            @pl.when(send_down_full)
            def _():
                down_copy(i, width).start()

            @pl.when(send_up_full)
            def _():
                up_copy(i, 0).start()

            @pl.when(i < EARLY)
            def _():
                send_far(i)

        @pl.when(k == hold)
        def _():
            pl.semaphore_wait(barrier, greetings)
            loop(0, hold, send)

        @pl.when(k >= hold)
        def _():
            send(k)

    loop(0, NP, first_pass)

    def stat_copy(d, slot):
        return pltpu.make_async_remote_copy(
            src_ref=gat.at[slot],
            dst_ref=gat.at[slot],
            send_sem=stat_send.at[d],
            recv_sem=stat_recv.at[slot],
            device_id={"samples": lax.rem(s + d, S)},
            device_id_type=MESH,
        )

    def tally_copy(d, slot):
        return pltpu.make_async_remote_copy(
            src_ref=tally.at[slot],
            dst_ref=tally.at[slot],
            send_sem=tally_send.at[d],
            recv_sem=tally_recv.at[slot],
            device_id={"samples": lax.rem(s + d, S)},
            device_id_type=MESH,
        )

    loop(1, S, lambda d: stat_copy(d, s).start())
    loop(1, S, lambda d: stat_copy(d, lax.rem(s + d, S)).wait_recv())

    sums = gat[0]
    for t in range(1, S):
        sums = sums + gat[t]
    w0, w1, w2 = sums[0:1], sums[1:2], sums[2:3]
    w_sum = w0 + w1 + w2
    mean = (w1 + 2.0 * w2) / w_sum
    one, two = 1.0 - mean, 2.0 - mean
    ms, os, ts = mean * mean, one * one, two * two
    var = (w0 * ms + w1 * os + w2 * ts) / w_sum
    factor = 1.0 / jnp.sqrt(w_sum * (var + 1e-05))
    par[0:1] = mean
    par[1:2] = factor
    for t in range(S):
        length = jnp.sqrt(gat[t, 0:1] * ms + gat[t, 1:2] * os + gat[t, 2:3] * ts)
        par[2 + t : 3 + t] = jnp.maximum(length * factor, 1e-12)
    spare = par.shape[0] - 2 - S
    if spare:
        par[2 + S :] = jnp.zeros((spare, rows), F32)

    def par_copy(i, dst, device):
        return pltpu.make_async_remote_copy(
            src_ref=par,
            dst_ref=dst,
            send_sem=par_send.at[i],
            recv_sem=par_recv.at[i],
            device_id={"variants": device},
            device_id_type=MESH,
        )

    @pl.when(has_prev)
    def _():
        par_copy(0, npar, down).start()

    @pl.when(from_prev)
    def _():
        par_copy(1, ppar, up).start()

    loop(EARLY, NP, send_far)

    stat_out[...] = jnp.concatenate([mean, var], axis=0)
    loop(1, S, lambda d: tally_copy(d, s).start())

    def start_build(src, col):
        aux[...] = jnp.concatenate([src[0:2], jnp.zeros((6, rows), F32)], axis=0)
        turned = aux[...].T
        for i in range(2):
            col[i] = jnp.broadcast_to(turned[:, i : i + 1], (rows, LANES))

    def build(src, col, lane):
        def of(who):
            line = jnp.zeros((1, rows), F32)
            for t in range(S):
                line = line + src[2 + t : 3 + t] * (who == t).astype(F32)
            return line

        mine, its = of(s), of(mate)
        both = jnp.sqrt(mine * mine + its * its)
        aux[...] = jnp.concatenate(
            [FULL / mine, its, FULL / both, jnp.zeros((5, rows), F32)], axis=0
        )
        turned = aux[...].T
        for i in range(3):
            col[2 + i] = jnp.broadcast_to(turned[:, i : i + 1], (rows, LANES))
        lane[0:1] = 1.0 / mine
        lane[1:2] = its * (1.0 / FULL)
        lane[2:3] = 1.0 / both

    def build_tall(src):
        sizes = []
        for q in range(PAIRS):
            a, b = src[2 + 2 * q : 3 + 2 * q], src[3 + 2 * q : 4 + 2 * q]
            sizes.append(jnp.sqrt(a * a + b * b))
        left = -PAIRS % 8
        if left:
            sizes.append(jnp.zeros((left, rows), F32))
        tall[:, 0 : PAIRS + left] = jnp.concatenate(sizes, axis=0).T

    def scale(src, src_row, dst, dst_row, count, lo, hi, col):
        def sixteen(i):
            here = pl.ds(aligned(src_row + i * STEP, STEP), STEP)
            there = pl.ds(aligned(dst_row + i * STEP, STEP), STEP)
            m, f = col[0, here], col[1, here]
            for b in range(lo // LANES, hi // LANES):
                lane = slice(b * LANES, (b + 1) * LANES)
                d = src[here, lane].astype(F32)
                r = jnp.broadcast_to(root[0:1, lane], (STEP, LANES))
                x = jnp.where(d < 2.5, r * (d - m) * f, 0.0).astype(BF16)
                dst[there, lane] = x

        loop(0, count // STEP, sixteen)

    def rows_of():
        row = lax.rem(s, H) * R
        for q in range(PAIRS):
            spread[q] = jnp.broadcast_to(
                tall[pl.ds(aligned(row, R), R), q : q + 1], (R, LANES)
            )

    start_build(par, col_o)
    scale(code, 0, scaled, 0, rows, 0, width, col_o)
    build(par, col_o, lane_o)

    def dot(a, b):
        return lax.dot_general(
            a, b, (((1,), (1,)), ((), ())), preferred_element_type=F32
        )

    def coded(value, e, line):
        q = jnp.round(value * e * line)
        q = jnp.clip(q, -32767.0, 32767.0)
        return q.astype(jnp.int32).astype(jnp.int16)

    def pack(src, src_row, col, col_row, lane, lane_at, cols, count, dst, dst_row):
        def sixteen(i):
            here = pl.ds(aligned(src_row + i * STEP, STEP), STEP)
            e = col[2, pl.ds(aligned(col_row + i * STEP, STEP), STEP)]
            for b in range(cols // LANES):
                part = slice(b * LANES, (b + 1) * LANES)
                line = lane[0:1, pl.ds(aligned(lane_at + b * LANES, LANES), LANES)]
                dst[pl.ds(aligned(dst_row + i * STEP, STEP), STEP), part] = coded(
                    src[here, part], e, line
                )

        loop(0, count // STEP, sixteen)

    def merge(
        src,
        src_row,
        got,
        got_row,
        col,
        col_row,
        lane,
        lane_at,
        cols,
        count,
        dst,
        dst_row,
        final,
    ):
        def sixteen(i):
            here = pl.ds(aligned(src_row + i * STEP, STEP), STEP)
            line_rows = pl.ds(aligned(col_row + i * STEP, STEP), STEP)
            there = pl.ds(aligned(dst_row + i * STEP, STEP), STEP)
            theirs = pl.ds(aligned(got_row + i * STEP, STEP), STEP)
            d, e = col[3, line_rows], col[4, line_rows]
            for b in range(cols // LANES):
                part = slice(b * LANES, (b + 1) * LANES)
                lanes = pl.ds(aligned(lane_at + b * LANES, LANES), LANES)
                q = got[theirs, part].astype(jnp.int32).astype(F32)
                value = src[here, part] + q * d * lane[1:2, lanes]
                if final:
                    dst[there, part] = value
                else:
                    dst[there, part] = coded(value, e, lane[2:3, lanes])

        loop(0, count // STEP, sixteen)

    def copy_to(src, dst, send, recv, device):
        return pltpu.make_async_remote_copy(
            src_ref=src,
            dst_ref=dst,
            send_sem=send,
            recv_sem=recv,
            device_id=device,
            device_id_type=MESH,
        )

    def yo_copy(j):
        return copy_to(
            ypart_o.at[j], yrcv_o.at[j], yo_send.at[j], yo_recv.at[j], {"samples": mate}
        )

    def zo_copy(j):
        return copy_to(
            zpart_o.at[j],
            zrcv.at[pair],
            zo_send.at[j],
            z_recv.at[pair],
            {"samples": 2 * j + y},
        )

    TALL = min(rows, 256)
    PER = TALL // R

    def own_rows(k):
        first = lax.rem(k * TALL + lax.div(turn * SUB, TALL) * TALL, rows)
        here = pl.ds(aligned(first, TALL), TALL)
        keep_o[here, :] = dot(scaled[here, :], scaled[...])

        def give(i):
            o = lax.div(first, R) + 2 * i + 1 - y
            j = lax.div(o, 2)
            pack(keep_o, o * R, col_o, o * R, lane_o, 0, rows, R, ypart_o.at[j], 0)
            yo_copy(j).start()

        loop(0, PER // 2, give)

    loop(0, rows // TALL, own_rows)

    mate_copy = copy_to(
        smp_mine,
        smp_mate,
        mate_send.at[0],
        mate_recv.at[0],
        {"variants": v + 1 - 2 * (v - 2 * chip)},
    )
    def squares(b):
        lanes = pl.ds(aligned(b * LANES, LANES), LANES)
        sums = [jnp.zeros((8, LANES), F32) for _ in range(4)]
        for i in range(rows // STEP):
            x = scaled[i * STEP : (i + 1) * STEP, lanes].astype(F32)
            x = x * x
            k = 2 * (i % 2)
            sums[k] = sums[k] + x[:8]
            sums[k + 1] = sums[k + 1] + x[8:]
        qacc[:, lanes] = (sums[0] + sums[1]) + (sums[2] + sums[3])

    def sample_sums():
        loop(0, blocks, squares)
        packed = sacc[...]
        tags = [
            jnp.bitwise_and(jnp.right_shift(packed, 8 * level), 255).astype(F32)
            for level in range(3)
        ]
        for q, value in enumerate([tags[0] + tags[1] + tags[2], tags[1], qacc[...]]):
            line = jnp.sum(value, axis=0, keepdims=True)
            for i in range(slabs):
                at = q * slabs + i
                smp_mine[at : at + 1, :] = line[:, i * SLAB : (i + 1) * SLAB]
        mate_copy.start()


    def smp_copy(d, slot):
        return copy_to(
            smp_all.at[slot],
            smp_all.at[slot],
            smp_send.at[d],
            smp_recv.at[slot],
            {"variants": lax.rem(v + 2 * d, V)},
        )

    def share_sums():
        mate_copy.wait_recv()
        smp_all[chip] = smp_mine[...] + smp_mate[...]
        loop(1, C, lambda d: smp_copy(d, chip).start())

    def own_norms():
        for q in range(PAIRS):
            a, b = par[2 + 2 * q : 3 + 2 * q], par[3 + 2 * q : 4 + 2 * q]
            lane_q[q] = jnp.sqrt(a * a + b * b) * (1.0 / FULL)

        @pl.when(s < H)
        def _():
            build_tall(par)
            rows_of()

    def rows_of():
        row = lax.rem(s, H) * R
        for q in range(PAIRS):
            spread[q] = jnp.broadcast_to(
                tall[pl.ds(aligned(row, R), R), q : q + 1], (R, LANES)
            )

    def collect_own(k):
        j = lax.rem(k + lax.div(turn * SUB, TALL) * (PER // 2), Q)
        o = 2 * j + y
        yo_copy(j).wait_recv()
        args = (keep_o, o * R, yrcv_o.at[j], 0, col_o, o * R, lane_o, 0, rows, R)

        @pl.when(o == s)
        def _():
            merge(*args, ld_out, 0, True)

        @pl.when(o != s)
        def _():
            merge(*args, zpart_o.at[j], 0, False)
            zo_copy(j).start()

    def yn_copy(at, size):
        j = lax.div(lax.div(at, R), 2)
        here = pl.ds(aligned(at - lax.div(at, R) * R, size), size)
        unit = lax.div(at, UNIT)
        return copy_to(
            ypart_n.at[j, here],
            yrcv_n.at[j, here],
            yn_send.at[unit],
            yn_recv.at[unit],
            {"samples": mate},
        )

    def zn_copy(at, size):
        r = lax.div(at, R)
        here = pl.ds(aligned(at - r * R, size), size)
        return copy_to(
            zpart_n.at[lax.div(r, 2), here],
            zrcv.at[pair, here],
            zn_send.at[lax.div(at, UNIT)],
            z_recv.at[pair],
            {"samples": H + r},
        )

    def next_rows(k, size):
        return lax.rem(k * size + lax.div(turn * SUB, size) * size, rows)

    def next_parity(at):
        r = lax.div(at, R)
        return r - 2 * lax.div(r, 2) == y

    def collect_next(at, size):
        r = lax.div(at, R)

        @pl.when(next_parity(at))
        def _():
            yn_copy(at, size).wait_recv()
            j = lax.div(r, 2)
            off = at - r * R
            args = (keep_x, at, yrcv_n.at[j], off, col_x, at, lane_o, 0, rows, size)

            @pl.when(H + r == s)
            def _():
                merge(*args, ld_out, off, True)

            @pl.when(H + r != s)
            def _():
                merge(*args, zpart_n.at[j], off, False)
                zn_copy(at, size).start()

    def give_next(at, size):
        r = lax.div(at, R)

        @pl.when(jnp.logical_not(next_parity(at)))
        def _():
            j = lax.div(r, 2)
            pack(
                keep_x, at, col_x, at, lane_o, 0, rows, size, ypart_n.at[j], at - r * R
            )
            yn_copy(at, size).start()

    def next_dot(at, tall_rows, hi):
        def arrived(i):
            down_copy(lax.rem(lax.div(at, SUB) + i + NP - turn, NP), hi).wait_recv()

        loop(0, tall_rows // SUB, arrived)
        scale(ncode, at, other, 0, tall_rows, 0, hi, col_x)
        here = pl.ds(aligned(at, tall_rows), tall_rows)
        keep_x[here, :] = dot(other[0:tall_rows, 0:hi], scaled[:, 0:hi])

    def next_role_full():
        pieces = TALL // R

        def each(at, act):
            loop(0, pieces, lambda i: act(at + i * R, R))

        count = rows // TALL
        for k in range(count):
            at = next_rows(k, TALL)
            next_dot(at, TALL, width)
            each(at, give_next)
            if k == 0:
                sample_sums()
                loop(0, Q, collect_own)
            else:
                each(next_rows(k - 1, TALL), collect_next)
        share_sums()
        own_norms()
        each(next_rows(count - 1, TALL), collect_next)
        next_norms()

    def next_role_part(hi):
        wide = LANES // UNIT
        count = rows // LANES

        def each(at, act):
            loop(0, wide, lambda i: act(at + i * UNIT, UNIT))

        def middle():
            sample_sums()
            loop(0, Q, collect_own)
            share_sums()
            own_norms()

        def chunk(k):
            at = next_rows(k, LANES)
            next_dot(at, LANES, hi)
            each(at, give_next)

            @pl.when(jnp.logical_and(k == 1, jnp.logical_not(does_full)))
            def _():
                middle()

            @pl.when(k > 0)
            def _():
                each(next_rows(k - 1, LANES), collect_next)

        loop(0, count - 1, chunk)
        next_norms()

        def small(k):
            at = next_rows(count - 1, LANES) + k * UNIT
            next_dot(at, UNIT, hi)
            give_next(at, UNIT)

            @pl.when(k == 0)
            def _():
                each(next_rows(count - 2, LANES), collect_next)

            @pl.when(k > 0)
            def _():
                collect_next(at - UNIT, UNIT)

        loop(0, wide, small)
        collect_next(next_rows(count - 1, LANES) + LANES - UNIT, UNIT)

    def yp_copy(c):
        return copy_to(
            ypart_p.at[c], yrcv_p.at[c], yp_send.at[c], yp_recv.at[c], {"samples": mate}
        )

    def zp_copy(j, c):
        return copy_to(
            zpart_p.at[j, c],
            zrcv_p.at[pair, c],
            zp_send.at[j],
            zp_recv.at[pair],
            {"samples": H + 2 * j + y, "variants": down},
        )

    def collect_prev(c):
        yp_copy(c).wait_recv()

        def one(i):
            j = lax.rem(i + pair, Q)
            o = (2 * j + y) * R
            merge(
                keep_x,
                c * rows + o,
                yrcv_p.at[c, j],
                0,
                col_o,
                o,
                lane_x,
                c * LANES,
                LANES,
                R,
                zpart_p.at[j, c],
                0,
                False,
            )
            zp_copy(j, c).start()

        loop(0, Q, one)

    def prev_dot(c, wide, lo):
        def arrived(i):
            up_copy(lax.rem(c * GROUP + i + NP - turn, NP), lo).wait_recv()

        loop(0, wide * GROUP, arrived)
        scale(pcode, c * LANES, other, 0, wide * LANES, lo, width, col_x)
        got = dot(scaled[:, lo:width], other[0 : wide * LANES, lo:width])
        for i in range(wide):
            here = pl.ds(aligned((c + i) * rows, rows), rows)
            keep_x[here, 0:LANES] = got[:, i * LANES : (i + 1) * LANES]

    def give_prev(c):
        def one(j):
            o = (2 * j + 1 - y) * R
            pack(
                keep_x,
                c * rows + o,
                col_o,
                o,
                lane_x,
                c * LANES,
                LANES,
                R,
                ypart_p.at[c, j],
                0,
            )

        loop(0, Q, one)
        yp_copy(c).start()

    def prev_role(wide, lo, full):
        count = NCP // wide
        first = lax.div(lax.div(turn, GROUP), wide)

        def at(k):
            return lax.rem(k + first, count) * wide

        def each(k, act):
            loop(0, wide, lambda i: act(at(k) + i))

        def chunk(k):
            prev_dot(at(k), wide, lo)
            each(k, give_prev)

        def middle():
            sample_sums()
            loop(0, Q, collect_own)
            share_sums()
            own_norms()

        if full:
            chunk(0)
            middle()
        else:
            chunk(0)
            chunk(1)

            @pl.when(jnp.logical_not(does_full))
            def _():
                middle()

            each(0, collect_prev)

        def rest(k):
            chunk(k)
            each(k - 1, collect_prev)

        loop(1 if full else 2, count, rest)
        each(count - 1, collect_prev)

    def with_next():
        par_copy(0, npar, down).wait_recv()
        start_build(npar, col_x)
        build(npar, col_x, lane_x)

    def next_norms():
        @pl.when(s >= H)
        def _():
            build_tall(npar)
            rows_of()


    def with_prev():
        par_copy(1, ppar, up).wait_recv()
        start_build(ppar, col_x)
        build(ppar, col_x, lane_x)


    @pl.when(prev_full)
    def _():
        with_prev()
        prev_role(min(2, NCP), 0, True)

    @pl.when(next_full)
    def _():
        with_next()
        next_role_full()

    @pl.when(prev_part)
    def _():
        with_prev()
        prev_role(1, KL, False)

    @pl.when(next_part)
    def _():
        with_next()
        next_role_part(KL)

    @pl.when(jnp.logical_and(jnp.logical_not(from_next), has_next))
    def _():
        par_copy(0, npar, down).wait_recv()
        next_norms()

    loop(1, S, lambda d: tally_copy(d, lax.rem(s + d, S)).wait_recv())
    counts = tally[0]
    for t in range(1, S):
        counts = counts + tally[t]
    count_out[...] = counts.astype(jnp.int32)

    loop(1, C, lambda d: smp_copy(d, lax.rem(chip + d, C)).wait_recv())
    all_sums = smp_all[0]
    for t in range(1, C):
        all_sums = all_sums + smp_all[t]
    call_out[...] = all_sums[: 2 * slabs].astype(jnp.int32)
    share_out[...] = all_sums[2 * slabs :] * F32((width * S) / (rows * V))

    def gather(got, q, part, wide):
        def sixteen(i):
            here = pl.ds(aligned(i * STEP, STEP), STEP)
            e = spread[q, here]
            for b in range(rows // LANES):
                lanes = slice(b * LANES, (b + 1) * LANES)
                line = lane_q[q, 0:1, lanes]
                piece = got[b, here] if wide else got[here, lanes]
                ld_out[here, lanes] += piece.astype(jnp.int32).astype(F32) * e * line

        loop(0, R // STEP, sixteen)

    def gather_pairs(d):
        q = lax.rem(pair + d, PAIRS)
        copy_to(
            zrcv.at[q], zrcv.at[q], zo_send.at[0], z_recv.at[q], {"samples": mate}
        ).wait_recv()
        gather(zrcv.at[q], q, None, False)

    def gather_prev(d):
        q = lax.rem(pair + d, PAIRS)
        copy_to(
            zrcv_p.at[q], zrcv_p.at[q], zp_send.at[0], zp_recv.at[q], {"samples": mate}
        ).wait_recv()
        gather(zrcv_p.at[q], q, None, True)

    @pl.when(s < H)
    def _():
        loop(1, PAIRS, gather_pairs)

    @pl.when(s >= H)
    def _():
        @pl.when(from_next)
        def _():
            loop(1, PAIRS, gather_pairs)

        @pl.when(jnp.logical_not(from_next))
        def _():
            ld_out[...] = jnp.zeros_like(ld_out)

        @pl.when(from_prev)
        def _():
            loop(0, PAIRS, gather_prev)

    loop(1, S, lambda d: stat_copy(d, s).wait_send())
    loop(1, S, lambda d: tally_copy(d, s).wait_send())
    loop(1, C, lambda d: smp_copy(d, chip).wait_send())
    mate_copy.wait_send()

    def drain_own(j):
        yo_copy(j).wait_send()

        @pl.when(2 * j + y != s)
        def _():
            zo_copy(j).wait_send()

    loop(0, Q, drain_own)

    def drain_next(size):
        def one(k):
            at = k * size
            mine = next_parity(at)

            @pl.when(jnp.logical_not(mine))
            def _():
                yn_copy(at, size).wait_send()

            @pl.when(jnp.logical_and(mine, H + lax.div(at, R) != s))
            def _():
                zn_copy(at, size).wait_send()

        loop(0, rows // size, one)

    @pl.when(next_full)
    def _():
        drain_next(R)

    @pl.when(next_part)
    def _():
        drain_next(UNIT)

    @pl.when(does_prev)
    def _():
        loop(0, NCP, lambda c: yp_copy(c).wait_send())

        def drain(j):
            copy_to(
                zpart_p.at[j], zpart_p.at[j], zp_send.at[j], zp_recv.at[0], {"samples": mate}
            ).wait_send()

        loop(0, Q, drain)

    @pl.when(has_prev)
    def _():
        par_copy(0, npar, down).wait_send()

    @pl.when(from_prev)
    def _():
        par_copy(1, ppar, up).wait_send()

    @pl.when(send_down_full)
    def _():
        loop(0, NP, lambda i: down_copy(i, width).wait_send())

    @pl.when(send_down_part)
    def _():
        loop(0, NP, lambda i: down_copy(i, KL).wait_send())

    @pl.when(send_up_full)
    def _():
        loop(0, NP, lambda i: up_copy(i, 0).wait_send())

    @pl.when(send_up_part)
    def _():
        loop(0, NP, lambda i: up_copy(i, KL).wait_send())


def finish(stats, counts, ld, calls, share, mean, var, counts_o, ld_o, calls_o, share_o):
    slabs = share.shape[0]
    mean[...] = stats[0]
    var[...] = stats[1]
    counts_o[...] = counts[...]
    ld_o[...] = ld[...]
    for i in range(slabs):
        here = slice(i * SLAB, (i + 1) * SLAB)
        for q in range(2):
            calls_o[q : q + 1, here] = calls[q * slabs + i : q * slabs + i + 1]
        share_o[here] = share[i]


def on_device(S, V, genotypes, weights):
    rows, width = genotypes.shape
    R = 2 * rows // S
    H = S // 2
    Q = H // 2
    PAIRS = S // 2
    C = V // 2
    NP = rows // SUB
    NCP = rows // LANES
    units = rows // min(R, 64)
    lines = -(-(2 + S) // 8) * 8
    slabs = width // SLAB
    vmem = pl.BlockSpec(memory_space=pltpu.VMEM)
    dma = pltpu.SemaphoreType.DMA
    stats, counts, ld, calls, share = pl.pallas_call(
        functools.partial(kernel, S, V),
        out_shape=(
            jax.ShapeDtypeStruct((2, rows), F32),
            jax.ShapeDtypeStruct((4, rows), jnp.int32),
            jax.ShapeDtypeStruct((R, rows), F32),
            jax.ShapeDtypeStruct((2 * slabs, SLAB), jnp.int32),
            jax.ShapeDtypeStruct((slabs, SLAB), F32),
        ),
        in_specs=[pl.BlockSpec(memory_space=pl.ANY)] * 2,
        out_specs=(vmem,) * 5,
        scratch_shapes=[
            pltpu.VMEM((rows, width), jnp.int32),
            pltpu.VMEM((rows, width), BF16),
            pltpu.VMEM((rows, width), BF16),
            pltpu.VMEM((rows, width), BF16),
            pltpu.VMEM((rows, width), BF16),
            pltpu.VMEM((min(rows, 256), width), BF16),
            pltpu.VMEM((rows, rows), F32),
            pltpu.VMEM((NCP * rows, rows), F32),
            pltpu.VMEM((Q, R, rows), jnp.int16),
            pltpu.VMEM((Q, R, rows), jnp.int16),
            pltpu.VMEM((Q, R, rows), jnp.int16),
            pltpu.VMEM((Q, R, rows), jnp.int16),
            pltpu.VMEM((NCP, Q, R, LANES), jnp.int16),
            pltpu.VMEM((NCP, Q, R, LANES), jnp.int16),
            pltpu.VMEM((Q, R, rows), jnp.int16),
            pltpu.VMEM((Q, R, rows), jnp.int16),
            pltpu.VMEM((Q, NCP, R, LANES), jnp.int16),
            pltpu.VMEM((PAIRS, R, rows), jnp.int16),
            pltpu.VMEM((PAIRS, NCP, R, LANES), jnp.int16),
            pltpu.VMEM((3, rows, LANES), F32),
            pltpu.VMEM((rows, LANES), jnp.int32),
            pltpu.VMEM((8, width), jnp.int32),
            pltpu.VMEM((8, width), F32),
            pltpu.VMEM((1, width), F32),
            pltpu.VMEM((S, 3, rows), F32),
            pltpu.VMEM((S, 4, rows), F32),
            pltpu.VMEM((lines, rows), F32),
            pltpu.VMEM((lines, rows), F32),
            pltpu.VMEM((lines, rows), F32),
            pltpu.VMEM((8, rows), F32),
            pltpu.VMEM((5, rows, LANES), F32),
            pltpu.VMEM((5, rows, LANES), F32),
            pltpu.VMEM((8, rows), F32),
            pltpu.VMEM((8, rows), F32),
            pltpu.VMEM((PAIRS, 1, rows), F32),
            pltpu.VMEM((rows, LANES), F32),
            pltpu.VMEM((PAIRS, R, LANES), F32),
            pltpu.VMEM((3 * slabs, SLAB), F32),
            pltpu.VMEM((3 * slabs, SLAB), F32),
            pltpu.VMEM((C, 3 * slabs, SLAB), F32),
            pltpu.VMEM((1, width), F32),
            dma((NP,)),
            dma(()),
            dma((NP,)),
            dma((NP,)),
            dma((NP,)),
            dma((NP,)),
            dma((S,)),
            dma((S,)),
            dma((S,)),
            dma((S,)),
            dma((2,)),
            dma((2,)),
            dma((Q,)),
            dma((Q,)),
            dma((units,)),
            dma((units,)),
            dma((NCP,)),
            dma((NCP,)),
            dma((Q,)),
            dma((units,)),
            dma((Q,)),
            dma((PAIRS,)),
            dma((PAIRS,)),
            dma((1,)),
            dma((1,)),
            dma((C,)),
            dma((C,)),
        ],
        compiler_params=pltpu.CompilerParams(
            collective_id=0, has_side_effects=True, vmem_limit_bytes=60 * 1024 * 1024
        ),
        name="window_stats",
    )(genotypes, weights.reshape(1, width))
    return pl.pallas_call(
        finish,
        out_shape=(
            jax.ShapeDtypeStruct((rows,), F32),
            jax.ShapeDtypeStruct((rows,), F32),
            jax.ShapeDtypeStruct((4, rows), jnp.int32),
            jax.ShapeDtypeStruct((R, rows), F32),
            jax.ShapeDtypeStruct((2, width), jnp.int32),
            jax.ShapeDtypeStruct((width,), F32),
        ),
        in_specs=[vmem] * 5,
        out_specs=(vmem,) * 6,
        name="finish",
    )(stats, counts, ld, calls, share)


def solution(mesh):
    body = functools.partial(on_device, mesh.shape["samples"], mesh.shape["variants"])
    return jax.shard_map(
        body,
        mesh=mesh,
        in_specs=(P("variants", "samples"), P("samples")),
        out_specs=(
            P("variants"),
            P("variants"),
            P(None, "variants"),
            P("samples", "variants"),
            P(None, "samples"),
            P("samples"),
        ),
        check_vma=False,
    )
```

```python
import functools

import jax
import jax.numpy as jnp
from jax import lax
from jax.experimental import pallas as pl
from jax.experimental.pallas import tpu as pltpu
from jax.sharding import PartitionSpec as P

MESH = pl.DeviceIdType.MESH
F32 = jnp.float32
BF16 = jnp.bfloat16
LANES = 128
STEP = 16
SUB = 32
FULL = 32400.0
SLAB = 512
EARLY = 7
LEFT = 16


def aligned(x, n):
    return pl.multiple_of(x, n)


def kernel(
    S,
    V,
    gen_hbm,
    w_hbm,
    stat_out,
    count_out,
    ld_out,
    call_out,
    share_out,
    gen,
    code,
    ncode,
    pcode,
    scaled,
    other,
    keep_o,
    keep_x,
    ypart_o,
    yrcv_o,
    ypart_n,
    yrcv_n,
    ypart_p,
    yrcv_p,
    zpart_o,
    zpart_n,
    zpart_p,
    zrcv,
    zrcv_p,
    wacc,
    cacc,
    sacc,
    qacc,
    root,
    gat,
    tally,
    par,
    npar,
    ppar,
    aux,
    col_o,
    col_x,
    lane_o,
    lane_x,
    lane_q,
    tall,
    spread,
    smp_mine,
    smp_mate,
    smp_all,
    w_ref,
    gen_sem,
    w_sem,
    ncode_send,
    ncode_recv,
    pcode_send,
    pcode_recv,
    stat_send,
    stat_recv,
    tally_send,
    tally_recv,
    par_send,
    par_recv,
    yo_send,
    yo_recv,
    yn_send,
    yn_recv,
    yp_send,
    yp_recv,
    zo_send,
    zn_send,
    zp_send,
    z_recv,
    zp_recv,
    mate_send,
    mate_recv,
    smp_send,
    smp_recv,
):
    s = lax.axis_index("samples")
    v = lax.axis_index("variants")
    rows, width = gen.shape
    R = 2 * rows // S
    H = S // 2
    Q = H // 2
    PAIRS = S // 2
    NP = rows // SUB
    GROUP = LANES // SUB
    UNIT = min(R, 64)
    NCP = rows // LANES
    KL = width * LEFT // 32 // LANES * LANES
    C = V // 2
    blocks = width // LANES
    slabs = width // SLAB

    pair = lax.div(s, 2)
    y = s - 2 * pair
    mate = s + 1 - 2 * y
    chip = lax.div(v, 2)
    odd = v - 2 * chip == 1
    even = jnp.logical_not(odd)
    near = 2 * chip < C
    far = jnp.logical_not(near)
    has_next = v < V - 1
    has_prev = v > 0
    next_part = jnp.logical_and(odd, has_next)
    next_full = jnp.logical_and(even, near)
    prev_part = jnp.logical_and(even, has_prev)
    prev_full = jnp.logical_and(odd, far)
    send_down_full = jnp.logical_and(odd, near)
    send_down_part = prev_part
    send_up_full = jnp.logical_and(even, far)
    send_up_part = next_part
    from_next = jnp.logical_or(next_part, next_full)
    from_prev = jnp.logical_or(send_up_full, send_up_part)
    does_prev = jnp.logical_or(prev_part, prev_full)
    does_full = jnp.logical_or(next_full, prev_full)
    hold = jnp.where(s == 0, 10, jnp.where(s < H, 5, 1))
    down = lax.rem(v + V - 1, V)
    up = lax.rem(v + 1, V)
    turn = lax.div(lax.div(pair * NP, PAIRS), 4) * 4

    def piece_rows(i):
        return pl.ds(aligned(lax.rem(i + turn, NP) * SUB, SUB), SUB)

    def load(i):
        return pltpu.make_async_copy(
            gen_hbm.at[piece_rows(i)], gen.at[piece_rows(i)], gen_sem.at[i]
        )

    def loop(start, stop, body):
        def step(i, _):
            body(i)
            return 0

        lax.fori_loop(start, stop, step, 0)

    w_load = pltpu.make_async_copy(w_hbm, w_ref, w_sem)
    load(0).start()
    w_load.start()
    loop(1, NP, lambda i: load(i).start())

    barrier = pltpu.get_barrier_semaphore()

    def greet(device):
        pl.semaphore_signal(barrier, inc=1, device_id=device, device_id_type=MESH)

    loop(1, S, lambda d: greet({"samples": lax.rem(s + d, S)}))
    loop(1, V, lambda d: greet({"variants": lax.rem(v + d, V)}))

    def cross_greet(d):
        there = 2 * lax.rem(pair + d, PAIRS) + y

        @pl.when(has_prev)
        def _():
            greet({"samples": there, "variants": down})

        @pl.when(has_next)
        def _():
            greet({"samples": there, "variants": up})

    loop(1, PAIRS, cross_greet)
    greetings = (
        S
        + V
        - 2
        + (PAIRS - 1) * (has_prev.astype(jnp.int32) + has_next.astype(jnp.int32))
    )

    sacc[...] = jnp.zeros_like(sacc)
    w_load.wait()
    root[...] = jnp.sqrt(w_ref[...])

    def piece_copy(i, buf, send, recv, device, lo, hi):
        here = piece_rows(i)
        return pltpu.make_async_remote_copy(
            src_ref=code.at[here, lo:hi],
            dst_ref=buf.at[here, lo:hi],
            send_sem=send.at[lax.rem(i + turn, NP)],
            recv_sem=recv.at[lax.rem(i + turn, NP)],
            device_id={"variants": device},
            device_id_type=MESH,
        )

    def down_copy(i, hi):
        return piece_copy(i, ncode, ncode_send, ncode_recv, down, 0, hi)

    def up_copy(i, lo):
        return piece_copy(i, pcode, pcode_send, pcode_recv, up, lo, width)

    def send_far(i):
        @pl.when(send_down_part)
        def _():
            down_copy(i, KL).start()

        @pl.when(send_up_part)
        def _():
            up_copy(i, KL).start()

    def total(x):
        return jnp.sum(x.T, axis=0, keepdims=True)

    def first_pass(k):
        load(k).wait()
        base = lax.rem(k + turn, NP) * SUB

        def sixteen(i):
            here = pl.ds(aligned(base + i * STEP, STEP), STEP)
            zero = jnp.zeros((STEP, LANES), F32)
            w0, w1, w2 = zero, zero, zero
            cnt = jnp.zeros((STEP, LANES), jnp.int32)
            for b in range(blocks):
                lane = slice(b * LANES, (b + 1) * LANES)
                g = gen[here, lane]
                w = jnp.broadcast_to(w_ref[0:1, lane], (STEP, LANES))
                w0 = w0 + jnp.where(g == 0, w, 0.0)
                w1 = w1 + jnp.where(g == 1, w, 0.0)
                w2 = w2 + jnp.where(g == 2, w, 0.0)
                tag = jnp.left_shift(jnp.int32(1), jnp.left_shift(g, 3))
                cnt = cnt + tag
                sacc[:, lane] += tag[:8] + tag[8:]
                code[here, lane] = g.astype(F32).astype(BF16)
            wacc[0, here] = w0
            wacc[1, here] = w1
            wacc[2, here] = w2
            cacc[here] = cnt

        loop(0, SUB // STEP, sixteen)

        @pl.when(lax.rem(k, GROUP) == GROUP - 1)
        def _():
            group = pl.ds(aligned(base + SUB - LANES, LANES), LANES)
            for i in range(3):
                gat[s, i : i + 1, group] = total(wacc[i, group])
            cnt = cacc[group]
            for level in range(4):
                some = jnp.bitwise_and(jnp.right_shift(cnt, 8 * level), 255)
                tally[s, level : level + 1, group] = total(some.astype(F32))

        def send(i):
            @pl.when(send_down_full)
            def _():
                down_copy(i, width).start()

            @pl.when(send_up_full)
            def _():
                up_copy(i, 0).start()

            @pl.when(i < EARLY)
            def _():
                send_far(i)

        @pl.when(k == hold)
        def _():
            pl.semaphore_wait(barrier, greetings)
            loop(0, hold, send)

        @pl.when(k >= hold)
        def _():
            send(k)

    loop(0, NP, first_pass)

    def stat_copy(d, slot):
        return pltpu.make_async_remote_copy(
            src_ref=gat.at[slot],
            dst_ref=gat.at[slot],
            send_sem=stat_send.at[d],
            recv_sem=stat_recv.at[slot],
            device_id={"samples": lax.rem(s + d, S)},
            device_id_type=MESH,
        )

    def tally_copy(d, slot):
        return pltpu.make_async_remote_copy(
            src_ref=tally.at[slot],
            dst_ref=tally.at[slot],
            send_sem=tally_send.at[d],
            recv_sem=tally_recv.at[slot],
            device_id={"samples": lax.rem(s + d, S)},
            device_id_type=MESH,
        )

    loop(1, S, lambda d: stat_copy(d, s).start())
    loop(1, S, lambda d: stat_copy(d, lax.rem(s + d, S)).wait_recv())

    sums = gat[0]
    for t in range(1, S):
        sums = sums + gat[t]
    w0, w1, w2 = sums[0:1], sums[1:2], sums[2:3]
    w_sum = w0 + w1 + w2
    mean = (w1 + 2.0 * w2) / w_sum
    one, two = 1.0 - mean, 2.0 - mean
    ms, os, ts = mean * mean, one * one, two * two
    var = (w0 * ms + w1 * os + w2 * ts) / w_sum
    factor = 1.0 / jnp.sqrt(w_sum * (var + 1e-05))
    par[0:1] = mean
    par[1:2] = factor
    for t in range(S):
        length = jnp.sqrt(gat[t, 0:1] * ms + gat[t, 1:2] * os + gat[t, 2:3] * ts)
        par[2 + t : 3 + t] = jnp.maximum(length * factor, 1e-12)
    spare = par.shape[0] - 2 - S
    if spare:
        par[2 + S :] = jnp.zeros((spare, rows), F32)

    def par_copy(i, dst, device):
        return pltpu.make_async_remote_copy(
            src_ref=par,
            dst_ref=dst,
            send_sem=par_send.at[i],
            recv_sem=par_recv.at[i],
            device_id={"variants": device},
            device_id_type=MESH,
        )

    @pl.when(has_prev)
    def _():
        par_copy(0, npar, down).start()

    @pl.when(from_prev)
    def _():
        par_copy(1, ppar, up).start()

    loop(EARLY, NP, send_far)

    stat_out[...] = jnp.concatenate([mean, var], axis=0)
    loop(1, S, lambda d: tally_copy(d, s).start())

    def start_build(src, col):
        aux[...] = jnp.concatenate([src[0:2], jnp.zeros((6, rows), F32)], axis=0)
        turned = aux[...].T
        for i in range(2):
            col[i] = jnp.broadcast_to(turned[:, i : i + 1], (rows, LANES))

    def build(src, col, lane):
        def of(who):
            line = jnp.zeros((1, rows), F32)
            for t in range(S):
                line = line + src[2 + t : 3 + t] * (who == t).astype(F32)
            return line

        mine, its = of(s), of(mate)
        both = jnp.sqrt(mine * mine + its * its)
        aux[...] = jnp.concatenate(
            [FULL / mine, its, FULL / both, jnp.zeros((5, rows), F32)], axis=0
        )
        turned = aux[...].T
        for i in range(3):
            col[2 + i] = jnp.broadcast_to(turned[:, i : i + 1], (rows, LANES))
        lane[0:1] = 1.0 / mine
        lane[1:2] = its * (1.0 / FULL)
        lane[2:3] = 1.0 / both

    def build_tall(src):
        sizes = []
        for q in range(PAIRS):
            a, b = src[2 + 2 * q : 3 + 2 * q], src[3 + 2 * q : 4 + 2 * q]
            sizes.append(jnp.sqrt(a * a + b * b))
        left = -PAIRS % 8
        if left:
            sizes.append(jnp.zeros((left, rows), F32))
        tall[:, 0 : PAIRS + left] = jnp.concatenate(sizes, axis=0).T

    def scale(src, src_row, dst, dst_row, count, lo, hi, col):
        def sixteen(i):
            here = pl.ds(aligned(src_row + i * STEP, STEP), STEP)
            there = pl.ds(aligned(dst_row + i * STEP, STEP), STEP)
            m, f = col[0, here], col[1, here]
            for b in range(lo // LANES, hi // LANES):
                lane = slice(b * LANES, (b + 1) * LANES)
                d = src[here, lane].astype(F32)
                r = jnp.broadcast_to(root[0:1, lane], (STEP, LANES))
                x = jnp.where(d < 2.5, r * (d - m) * f, 0.0).astype(BF16)
                dst[there, lane] = x

        loop(0, count // STEP, sixteen)

    def rows_of():
        row = lax.rem(s, H) * R
        for q in range(PAIRS):
            spread[q] = jnp.broadcast_to(
                tall[pl.ds(aligned(row, R), R), q : q + 1], (R, LANES)
            )

    start_build(par, col_o)
    scale(code, 0, scaled, 0, rows, 0, width, col_o)
    build(par, col_o, lane_o)

    def dot(a, b):
        return lax.dot_general(
            a, b, (((1,), (1,)), ((), ())), preferred_element_type=F32
        )

    def coded(value, e, line):
        q = jnp.round(value * e * line)
        q = jnp.clip(q, -32767.0, 32767.0)
        return q.astype(jnp.int32).astype(jnp.int16)

    def pack(src, src_row, col, col_row, lane, lane_at, cols, count, dst, dst_row):
        def sixteen(i):
            here = pl.ds(aligned(src_row + i * STEP, STEP), STEP)
            e = col[2, pl.ds(aligned(col_row + i * STEP, STEP), STEP)]
            for b in range(cols // LANES):
                part = slice(b * LANES, (b + 1) * LANES)
                line = lane[0:1, pl.ds(aligned(lane_at + b * LANES, LANES), LANES)]
                dst[pl.ds(aligned(dst_row + i * STEP, STEP), STEP), part] = coded(
                    src[here, part], e, line
                )

        loop(0, count // STEP, sixteen)

    def merge(
        src,
        src_row,
        got,
        got_row,
        col,
        col_row,
        lane,
        lane_at,
        cols,
        count,
        dst,
        dst_row,
        final,
    ):
        def sixteen(i):
            here = pl.ds(aligned(src_row + i * STEP, STEP), STEP)
            line_rows = pl.ds(aligned(col_row + i * STEP, STEP), STEP)
            there = pl.ds(aligned(dst_row + i * STEP, STEP), STEP)
            theirs = pl.ds(aligned(got_row + i * STEP, STEP), STEP)
            d, e = col[3, line_rows], col[4, line_rows]
            for b in range(cols // LANES):
                part = slice(b * LANES, (b + 1) * LANES)
                lanes = pl.ds(aligned(lane_at + b * LANES, LANES), LANES)
                q = got[theirs, part].astype(jnp.int32).astype(F32)
                value = src[here, part] + q * d * lane[1:2, lanes]
                if final:
                    dst[there, part] = value
                else:
                    dst[there, part] = coded(value, e, lane[2:3, lanes])

        loop(0, count // STEP, sixteen)

    def copy_to(src, dst, send, recv, device):
        return pltpu.make_async_remote_copy(
            src_ref=src,
            dst_ref=dst,
            send_sem=send,
            recv_sem=recv,
            device_id=device,
            device_id_type=MESH,
        )

    def yo_copy(j):
        return copy_to(
            ypart_o.at[j], yrcv_o.at[j], yo_send.at[j], yo_recv.at[j], {"samples": mate}
        )

    def zo_copy(j):
        return copy_to(
            zpart_o.at[j],
            zrcv.at[pair],
            zo_send.at[j],
            z_recv.at[pair],
            {"samples": 2 * j + y},
        )

    TALL = min(rows, 256)
    PER = TALL // R

    def own_rows(k):
        first = lax.rem(k * TALL + lax.div(turn * SUB, TALL) * TALL, rows)
        here = pl.ds(aligned(first, TALL), TALL)
        keep_o[here, :] = dot(scaled[here, :], scaled[...])

        def give(i):
            o = lax.div(first, R) + 2 * i + 1 - y
            j = lax.div(o, 2)
            pack(keep_o, o * R, col_o, o * R, lane_o, 0, rows, R, ypart_o.at[j], 0)
            yo_copy(j).start()

        loop(0, PER // 2, give)

    loop(0, rows // TALL, own_rows)

    mate_copy = copy_to(
        smp_mine,
        smp_mate,
        mate_send.at[0],
        mate_recv.at[0],
        {"variants": v + 1 - 2 * (v - 2 * chip)},
    )
    def squares(b):
        lanes = pl.ds(aligned(b * LANES, LANES), LANES)
        sums = [jnp.zeros((8, LANES), F32) for _ in range(4)]
        for i in range(rows // STEP):
            x = scaled[i * STEP : (i + 1) * STEP, lanes].astype(F32)
            x = x * x
            k = 2 * (i % 2)
            sums[k] = sums[k] + x[:8]
            sums[k + 1] = sums[k + 1] + x[8:]
        qacc[:, lanes] = (sums[0] + sums[1]) + (sums[2] + sums[3])

    def sample_sums():
        loop(0, blocks, squares)
        packed = sacc[...]
        tags = [
            jnp.bitwise_and(jnp.right_shift(packed, 8 * level), 255).astype(F32)
            for level in range(3)
        ]
        for q, value in enumerate([tags[0] + tags[1] + tags[2], tags[1], qacc[...]]):
            line = jnp.sum(value, axis=0, keepdims=True)
            for i in range(slabs):
                at = q * slabs + i
                smp_mine[at : at + 1, :] = line[:, i * SLAB : (i + 1) * SLAB]
        mate_copy.start()


    def smp_copy(d, slot):
        return copy_to(
            smp_all.at[slot],
            smp_all.at[slot],
            smp_send.at[d],
            smp_recv.at[slot],
            {"variants": lax.rem(v + 2 * d, V)},
        )

    def share_sums():
        mate_copy.wait_recv()
        smp_all[chip] = smp_mine[...] + smp_mate[...]
        loop(1, C, lambda d: smp_copy(d, chip).start())

    def own_norms():
        for q in range(PAIRS):
            a, b = par[2 + 2 * q : 3 + 2 * q], par[3 + 2 * q : 4 + 2 * q]
            lane_q[q] = jnp.sqrt(a * a + b * b) * (1.0 / FULL)

        @pl.when(s < H)
        def _():
            build_tall(par)
            rows_of()

    def rows_of():
        row = lax.rem(s, H) * R
        for q in range(PAIRS):
            spread[q] = jnp.broadcast_to(
                tall[pl.ds(aligned(row, R), R), q : q + 1], (R, LANES)
            )

    def own_half(i):
        loop(i * (Q // 2), (i + 1) * (Q // 2), collect_own)

    def collect_own(k):
        j = lax.rem(k + lax.div(turn * SUB, TALL) * (PER // 2), Q)
        o = 2 * j + y
        yo_copy(j).wait_recv()
        args = (keep_o, o * R, yrcv_o.at[j], 0, col_o, o * R, lane_o, 0, rows, R)

        @pl.when(o == s)
        def _():
            merge(*args, ld_out, 0, True)

        @pl.when(o != s)
        def _():
            merge(*args, zpart_o.at[j], 0, False)
            zo_copy(j).start()

    def yn_copy(at, size):
        j = lax.div(lax.div(at, R), 2)
        here = pl.ds(aligned(at - lax.div(at, R) * R, size), size)
        unit = lax.div(at, UNIT)
        return copy_to(
            ypart_n.at[j, here],
            yrcv_n.at[j, here],
            yn_send.at[unit],
            yn_recv.at[unit],
            {"samples": mate},
        )

    def zn_copy(at, size):
        r = lax.div(at, R)
        here = pl.ds(aligned(at - r * R, size), size)
        return copy_to(
            zpart_n.at[lax.div(r, 2), here],
            zrcv.at[pair, here],
            zn_send.at[lax.div(at, UNIT)],
            z_recv.at[pair],
            {"samples": H + r},
        )

    def next_rows(k, size):
        return lax.rem(k * size + lax.div(turn * SUB, size) * size, rows)

    def next_parity(at):
        r = lax.div(at, R)
        return r - 2 * lax.div(r, 2) == y

    def collect_next(at, size):
        r = lax.div(at, R)

        @pl.when(next_parity(at))
        def _():
            yn_copy(at, size).wait_recv()
            j = lax.div(r, 2)
            off = at - r * R
            args = (keep_x, at, yrcv_n.at[j], off, col_x, at, lane_o, 0, rows, size)

            @pl.when(H + r == s)
            def _():
                merge(*args, ld_out, off, True)

            @pl.when(H + r != s)
            def _():
                merge(*args, zpart_n.at[j], off, False)
                zn_copy(at, size).start()

    def give_next(at, size):
        r = lax.div(at, R)

        @pl.when(jnp.logical_not(next_parity(at)))
        def _():
            j = lax.div(r, 2)
            pack(
                keep_x, at, col_x, at, lane_o, 0, rows, size, ypart_n.at[j], at - r * R
            )
            yn_copy(at, size).start()

    def next_dot(at, tall_rows, hi):
        def arrived(i):
            down_copy(lax.rem(lax.div(at, SUB) + i + NP - turn, NP), hi).wait_recv()

        loop(0, tall_rows // SUB, arrived)
        scale(ncode, at, other, 0, tall_rows, 0, hi, col_x)
        here = pl.ds(aligned(at, tall_rows), tall_rows)
        keep_x[here, :] = dot(other[0:tall_rows, 0:hi], scaled[:, 0:hi])

    def next_role_full():
        pieces = TALL // R

        def each(at, act):
            loop(0, pieces, lambda i: act(at + i * R, R))

        count = rows // TALL
        for k in range(count):
            at = next_rows(k, TALL)
            next_dot(at, TALL, width)
            each(at, give_next)
            if k == 0:
                own_half(0)
            if k == count - 1:
                own_half(1)
            if k > 0:
                each(next_rows(k - 1, TALL), collect_next)
        sample_sums()
        each(next_rows(count - 1, TALL), collect_next)
        share_sums()
        own_norms()
        next_norms()

    def next_role_part(hi):
        wide = LANES // UNIT
        count = rows // LANES

        def each(at, act):
            loop(0, wide, lambda i: act(at + i * UNIT, UNIT))

        alone = jnp.logical_not(does_full)

        def chunk(k):
            at = next_rows(k, LANES)
            next_dot(at, LANES, hi)
            each(at, give_next)

            @pl.when(jnp.logical_and(k == 0, alone))
            def _():
                own_half(0)

            @pl.when(jnp.logical_and(k == 1, alone))
            def _():
                sample_sums()
                own_half(1)

            @pl.when(k > 0)
            def _():
                each(next_rows(k - 1, LANES), collect_next)

        loop(0, count - 1, chunk)
        next_norms()

        def small(k):
            at = next_rows(count - 1, LANES) + k * UNIT
            next_dot(at, UNIT, hi)
            give_next(at, UNIT)

            @pl.when(k == 0)
            def _():
                each(next_rows(count - 2, LANES), collect_next)

            @pl.when(k > 0)
            def _():
                collect_next(at - UNIT, UNIT)

        loop(0, wide, small)

        @pl.when(alone)
        def _():
            share_sums()
            own_norms()

        collect_next(next_rows(count - 1, LANES) + LANES - UNIT, UNIT)

    def yp_copy(c):
        return copy_to(
            ypart_p.at[c], yrcv_p.at[c], yp_send.at[c], yp_recv.at[c], {"samples": mate}
        )

    def zp_copy(j, c):
        return copy_to(
            zpart_p.at[j, c],
            zrcv_p.at[pair, c],
            zp_send.at[j],
            zp_recv.at[pair],
            {"samples": H + 2 * j + y, "variants": down},
        )

    def collect_prev(c):
        yp_copy(c).wait_recv()

        def one(i):
            j = lax.rem(i + pair, Q)
            o = (2 * j + y) * R
            merge(
                keep_x,
                c * rows + o,
                yrcv_p.at[c, j],
                0,
                col_o,
                o,
                lane_x,
                c * LANES,
                LANES,
                R,
                zpart_p.at[j, c],
                0,
                False,
            )
            zp_copy(j, c).start()

        loop(0, Q, one)

    def prev_dot(c, wide, lo):
        def arrived(i):
            up_copy(lax.rem(c * GROUP + i + NP - turn, NP), lo).wait_recv()

        loop(0, wide * GROUP, arrived)
        scale(pcode, c * LANES, other, 0, wide * LANES, lo, width, col_x)
        got = dot(scaled[:, lo:width], other[0 : wide * LANES, lo:width])
        for i in range(wide):
            here = pl.ds(aligned((c + i) * rows, rows), rows)
            keep_x[here, 0:LANES] = got[:, i * LANES : (i + 1) * LANES]

    def give_prev(c):
        def one(j):
            o = (2 * j + 1 - y) * R
            pack(
                keep_x,
                c * rows + o,
                col_o,
                o,
                lane_x,
                c * LANES,
                LANES,
                R,
                ypart_p.at[c, j],
                0,
            )

        loop(0, Q, one)
        yp_copy(c).start()

    def prev_role(wide, lo, full):
        count = NCP // wide
        first = lax.div(lax.div(turn, GROUP), wide)

        def at(k):
            return lax.rem(k + first, count) * wide

        def each(k, act):
            loop(0, wide, lambda i: act(at(k) + i))

        def chunk(k):
            prev_dot(at(k), wide, lo)
            each(k, give_prev)

        if full:
            chunk(0)
            own_half(0)
            chunk(1)
            own_half(1)
            each(0, collect_prev)
            sample_sums()
        else:
            alone = jnp.logical_not(does_full)
            chunk(0)

            @pl.when(alone)
            def _():
                own_half(0)

            chunk(1)

            @pl.when(alone)
            def _():
                own_half(1)

            each(0, collect_prev)

            @pl.when(alone)
            def _():
                sample_sums()

        def rest(k):
            chunk(k)
            each(k - 1, collect_prev)

        loop(2, count, rest)

        @pl.when(jnp.logical_or(full, jnp.logical_not(does_full)))
        def _():
            share_sums()
            own_norms()

        each(count - 1, collect_prev)

    def with_next():
        par_copy(0, npar, down).wait_recv()
        start_build(npar, col_x)
        build(npar, col_x, lane_x)

    def next_norms():
        @pl.when(s >= H)
        def _():
            build_tall(npar)
            rows_of()


    def with_prev():
        par_copy(1, ppar, up).wait_recv()
        start_build(ppar, col_x)
        build(ppar, col_x, lane_x)


    @pl.when(prev_full)
    def _():
        with_prev()
        prev_role(min(2, NCP), 0, True)

    @pl.when(next_full)
    def _():
        with_next()
        next_role_full()

    @pl.when(prev_part)
    def _():
        with_prev()
        prev_role(1, KL, False)

    @pl.when(next_part)
    def _():
        with_next()
        next_role_part(KL)

    @pl.when(jnp.logical_and(jnp.logical_not(from_next), has_next))
    def _():
        par_copy(0, npar, down).wait_recv()
        next_norms()

    loop(1, S, lambda d: stat_copy(d, s).wait_send())
    loop(1, S, lambda d: tally_copy(d, s).wait_send())
    mate_copy.wait_send()


    @pl.when(has_prev)
    def _():
        par_copy(0, npar, down).wait_send()

    @pl.when(from_prev)
    def _():
        par_copy(1, ppar, up).wait_send()

    @pl.when(send_down_full)
    def _():
        loop(0, NP, lambda i: down_copy(i, width).wait_send())

    @pl.when(send_down_part)
    def _():
        loop(0, NP, lambda i: down_copy(i, KL).wait_send())

    @pl.when(send_up_full)
    def _():
        loop(0, NP, lambda i: up_copy(i, 0).wait_send())

    @pl.when(send_up_part)
    def _():
        loop(0, NP, lambda i: up_copy(i, KL).wait_send())

    loop(1, S, lambda d: tally_copy(d, lax.rem(s + d, S)).wait_recv())
    counts = tally[0]
    for t in range(1, S):
        counts = counts + tally[t]
    count_out[...] = counts.astype(jnp.int32)

    loop(1, C, lambda d: smp_copy(d, lax.rem(chip + d, C)).wait_recv())
    all_sums = smp_all[0]
    for t in range(1, C):
        all_sums = all_sums + smp_all[t]
    call_out[...] = all_sums[: 2 * slabs].astype(jnp.int32)
    share_out[...] = all_sums[2 * slabs :] * F32((width * S) / (rows * V))

    def gather(got, q, part, wide):
        def sixteen(i):
            here = pl.ds(aligned(i * STEP, STEP), STEP)
            e = spread[q, here]
            for b in range(rows // LANES):
                lanes = slice(b * LANES, (b + 1) * LANES)
                line = lane_q[q, 0:1, lanes]
                piece = got[b, here] if wide else got[here, lanes]
                ld_out[here, lanes] += piece.astype(jnp.int32).astype(F32) * e * line

        loop(0, R // STEP, sixteen)

    def gather_pairs(d):
        q = lax.rem(pair + d, PAIRS)
        copy_to(
            zrcv.at[q], zrcv.at[q], zo_send.at[0], z_recv.at[q], {"samples": mate}
        ).wait_recv()
        gather(zrcv.at[q], q, None, False)

    def gather_prev(d):
        q = lax.rem(pair + d, PAIRS)
        copy_to(
            zrcv_p.at[q], zrcv_p.at[q], zp_send.at[0], zp_recv.at[q], {"samples": mate}
        ).wait_recv()
        gather(zrcv_p.at[q], q, None, True)

    @pl.when(s < H)
    def _():
        loop(1, PAIRS, gather_pairs)

    @pl.when(s >= H)
    def _():
        @pl.when(from_next)
        def _():
            loop(1, PAIRS, gather_pairs)

        @pl.when(jnp.logical_not(from_next))
        def _():
            ld_out[...] = jnp.zeros_like(ld_out)

        @pl.when(from_prev)
        def _():
            loop(0, PAIRS, gather_prev)

    def drain_own(j):
        yo_copy(j).wait_send()

        @pl.when(2 * j + y != s)
        def _():
            zo_copy(j).wait_send()

    loop(0, Q, drain_own)

    def drain_next(size):
        def one(k):
            at = k * size
            mine = next_parity(at)

            @pl.when(jnp.logical_not(mine))
            def _():
                yn_copy(at, size).wait_send()

            @pl.when(jnp.logical_and(mine, H + lax.div(at, R) != s))
            def _():
                zn_copy(at, size).wait_send()

        loop(0, rows // size, one)

    @pl.when(next_full)
    def _():
        drain_next(R)

    @pl.when(next_part)
    def _():
        drain_next(UNIT)

    @pl.when(does_prev)
    def _():
        loop(0, NCP, lambda c: yp_copy(c).wait_send())

        def drain(j):
            copy_to(
                zpart_p.at[j], zpart_p.at[j], zp_send.at[j], zp_recv.at[0], {"samples": mate}
            ).wait_send()

        loop(0, Q, drain)

    loop(1, C, lambda d: smp_copy(d, chip).wait_send())


def finish(stats, counts, ld, calls, share, mean, var, counts_o, ld_o, calls_o, share_o):
    slabs = share.shape[0]
    mean[...] = stats[0]
    var[...] = stats[1]
    counts_o[...] = counts[...]
    ld_o[...] = ld[...]
    for i in range(slabs):
        here = slice(i * SLAB, (i + 1) * SLAB)
        for q in range(2):
            calls_o[q : q + 1, here] = calls[q * slabs + i : q * slabs + i + 1]
        share_o[here] = share[i]


def on_device(S, V, genotypes, weights):
    rows, width = genotypes.shape
    R = 2 * rows // S
    H = S // 2
    Q = H // 2
    PAIRS = S // 2
    C = V // 2
    NP = rows // SUB
    NCP = rows // LANES
    units = rows // min(R, 64)
    lines = -(-(2 + S) // 8) * 8
    slabs = width // SLAB
    vmem = pl.BlockSpec(memory_space=pltpu.VMEM)
    dma = pltpu.SemaphoreType.DMA
    results = pl.pallas_call(
        functools.partial(kernel, S, V),
        out_shape=(
            pltpu.VMEM((2, rows), F32),
            pltpu.VMEM((4, rows), jnp.int32),
            pltpu.VMEM((R, rows), F32),
            pltpu.VMEM((2 * slabs, SLAB), jnp.int32),
            pltpu.VMEM((slabs, SLAB), F32),
        ),
        in_specs=[pl.BlockSpec(memory_space=pl.ANY)] * 2,
        out_specs=(vmem,) * 5,
        scratch_shapes=[
            pltpu.VMEM((rows, width), jnp.int32),
            pltpu.VMEM((rows, width), BF16),
            pltpu.VMEM((rows, width), BF16),
            pltpu.VMEM((rows, width), BF16),
            pltpu.VMEM((rows, width), BF16),
            pltpu.VMEM((min(rows, 256), width), BF16),
            pltpu.VMEM((rows, rows), F32),
            pltpu.VMEM((NCP * rows, rows), F32),
            pltpu.VMEM((Q, R, rows), jnp.int16),
            pltpu.VMEM((Q, R, rows), jnp.int16),
            pltpu.VMEM((Q, R, rows), jnp.int16),
            pltpu.VMEM((Q, R, rows), jnp.int16),
            pltpu.VMEM((NCP, Q, R, LANES), jnp.int16),
            pltpu.VMEM((NCP, Q, R, LANES), jnp.int16),
            pltpu.VMEM((Q, R, rows), jnp.int16),
            pltpu.VMEM((Q, R, rows), jnp.int16),
            pltpu.VMEM((Q, NCP, R, LANES), jnp.int16),
            pltpu.VMEM((PAIRS, R, rows), jnp.int16),
            pltpu.VMEM((PAIRS, NCP, R, LANES), jnp.int16),
            pltpu.VMEM((3, rows, LANES), F32),
            pltpu.VMEM((rows, LANES), jnp.int32),
            pltpu.VMEM((8, width), jnp.int32),
            pltpu.VMEM((8, width), F32),
            pltpu.VMEM((1, width), F32),
            pltpu.VMEM((S, 3, rows), F32),
            pltpu.VMEM((S, 4, rows), F32),
            pltpu.VMEM((lines, rows), F32),
            pltpu.VMEM((lines, rows), F32),
            pltpu.VMEM((lines, rows), F32),
            pltpu.VMEM((8, rows), F32),
            pltpu.VMEM((5, rows, LANES), F32),
            pltpu.VMEM((5, rows, LANES), F32),
            pltpu.VMEM((8, rows), F32),
            pltpu.VMEM((8, rows), F32),
            pltpu.VMEM((PAIRS, 1, rows), F32),
            pltpu.VMEM((rows, LANES), F32),
            pltpu.VMEM((PAIRS, R, LANES), F32),
            pltpu.VMEM((3 * slabs, SLAB), F32),
            pltpu.VMEM((3 * slabs, SLAB), F32),
            pltpu.VMEM((C, 3 * slabs, SLAB), F32),
            pltpu.VMEM((1, width), F32),
            dma((NP,)),
            dma(()),
            dma((NP,)),
            dma((NP,)),
            dma((NP,)),
            dma((NP,)),
            dma((S,)),
            dma((S,)),
            dma((S,)),
            dma((S,)),
            dma((2,)),
            dma((2,)),
            dma((Q,)),
            dma((Q,)),
            dma((units,)),
            dma((units,)),
            dma((NCP,)),
            dma((NCP,)),
            dma((Q,)),
            dma((units,)),
            dma((Q,)),
            dma((PAIRS,)),
            dma((PAIRS,)),
            dma((1,)),
            dma((1,)),
            dma((C,)),
            dma((C,)),
        ],
        compiler_params=pltpu.CompilerParams(
            collective_id=0, has_side_effects=True, vmem_limit_bytes=60 * 1024 * 1024
        ),
        name="window_stats",
    )(genotypes, weights.reshape(1, width))
    results = [pltpu.with_memory_space_constraint(x, pltpu.VMEM) for x in results]
    return pl.pallas_call(
        finish,
        out_shape=(
            jax.ShapeDtypeStruct((rows,), F32),
            jax.ShapeDtypeStruct((rows,), F32),
            jax.ShapeDtypeStruct((4, rows), jnp.int32),
            jax.ShapeDtypeStruct((R, rows), F32),
            jax.ShapeDtypeStruct((2, width), jnp.int32),
            jax.ShapeDtypeStruct((width,), F32),
        ),
        in_specs=[vmem] * 5,
        out_specs=(vmem,) * 6,
        name="finish",
    )(*results)


def solution(mesh):
    body = functools.partial(on_device, mesh.shape["samples"], mesh.shape["variants"])
    return jax.shard_map(
        body,
        mesh=mesh,
        in_specs=(P("variants", "samples"), P("samples")),
        out_specs=(
            P("variants"),
            P("variants"),
            P(None, "variants"),
            P("samples", "variants"),
            P(None, "samples"),
            P("samples"),
        ),
        check_vma=False,
    )
```

```python
import functools

import jax
import jax.numpy as jnp
from jax import lax
from jax.experimental import pallas as pl
from jax.experimental.pallas import tpu as pltpu
from jax.sharding import PartitionSpec as P

MESH = pl.DeviceIdType.MESH
F32 = jnp.float32
BF16 = jnp.bfloat16
LANES = 128
STEP = 16
SUB = 32
FULL = 32400.0
SLAB = 512
EARLY = 7
LEFT = 16


def aligned(x, n):
    return pl.multiple_of(x, n)


def kernel(
    S,
    V,
    gen_hbm,
    w_hbm,
    stat_out,
    count_out,
    ld_out,
    call_out,
    share_out,
    gen,
    code,
    ncode,
    pcode,
    scaled,
    other,
    keep_o,
    keep_x,
    ypart_o,
    yrcv_o,
    ypart_n,
    yrcv_n,
    ypart_p,
    yrcv_p,
    zpart_o,
    zpart_n,
    zpart_p,
    zrcv,
    zrcv_p,
    wacc,
    cacc,
    sacc,
    qacc,
    root,
    gat,
    tally,
    par,
    npar,
    ppar,
    aux,
    col_o,
    col_x,
    lane_o,
    lane_x,
    lane_q,
    tall,
    spread,
    smp_mine,
    smp_mate,
    smp_all,
    w_ref,
    gen_sem,
    w_sem,
    ncode_send,
    ncode_recv,
    pcode_send,
    pcode_recv,
    stat_send,
    stat_recv,
    tally_send,
    tally_recv,
    par_send,
    par_recv,
    yo_send,
    yo_recv,
    yn_send,
    yn_recv,
    yp_send,
    yp_recv,
    zo_send,
    zn_send,
    zp_send,
    z_recv,
    zp_recv,
    mate_send,
    mate_recv,
    smp_send,
    smp_recv,
):
    s = lax.axis_index("samples")
    v = lax.axis_index("variants")
    rows, width = gen.shape
    R = 2 * rows // S
    H = S // 2
    Q = H // 2
    PAIRS = S // 2
    NP = rows // SUB
    GROUP = LANES // SUB
    UNIT = min(R, 64)
    NCP = rows // LANES
    KL = width * LEFT // 32 // LANES * LANES
    C = V // 2
    blocks = width // LANES
    slabs = width // SLAB

    pair = lax.div(s, 2)
    y = s - 2 * pair
    mate = s + 1 - 2 * y
    chip = lax.div(v, 2)
    odd = v - 2 * chip == 1
    even = jnp.logical_not(odd)
    near = 2 * chip < C
    far = jnp.logical_not(near)
    has_next = v < V - 1
    has_prev = v > 0
    next_part = jnp.logical_and(odd, has_next)
    next_full = jnp.logical_and(even, near)
    prev_part = jnp.logical_and(even, has_prev)
    prev_full = jnp.logical_and(odd, far)
    send_down_full = jnp.logical_and(odd, near)
    send_down_part = prev_part
    send_up_full = jnp.logical_and(even, far)
    send_up_part = next_part
    from_next = jnp.logical_or(next_part, next_full)
    from_prev = jnp.logical_or(send_up_full, send_up_part)
    does_prev = jnp.logical_or(prev_part, prev_full)
    does_full = jnp.logical_or(next_full, prev_full)
    hold = jnp.where(s == 0, 12, jnp.where(s < H, 7, 3))
    down = lax.rem(v + V - 1, V)
    up = lax.rem(v + 1, V)
    turn = lax.div(lax.div(pair * NP, PAIRS), 4) * 4

    def piece_rows(i):
        return pl.ds(aligned(lax.rem(i + turn, NP) * SUB, SUB), SUB)

    def load(i):
        return pltpu.make_async_copy(
            gen_hbm.at[piece_rows(i)], gen.at[piece_rows(i)], gen_sem.at[i]
        )

    def loop(start, stop, body):
        def step(i, _):
            body(i)
            return 0

        lax.fori_loop(start, stop, step, 0)

    w_load = pltpu.make_async_copy(w_hbm, w_ref, w_sem)
    load(0).start()
    w_load.start()
    loop(1, NP, lambda i: load(i).start())

    barrier = pltpu.get_barrier_semaphore()

    def greet(device):
        pl.semaphore_signal(barrier, inc=1, device_id=device, device_id_type=MESH)

    loop(1, S, lambda d: greet({"samples": lax.rem(s + d, S)}))
    loop(1, V, lambda d: greet({"variants": lax.rem(v + d, V)}))

    def cross_greet(d):
        there = 2 * lax.rem(pair + d, PAIRS) + y

        @pl.when(has_prev)
        def _():
            greet({"samples": there, "variants": down})

        @pl.when(has_next)
        def _():
            greet({"samples": there, "variants": up})

    loop(1, PAIRS, cross_greet)
    greetings = (
        S
        + V
        - 2
        + (PAIRS - 1) * (has_prev.astype(jnp.int32) + has_next.astype(jnp.int32))
    )

    sacc[...] = jnp.zeros_like(sacc)
    w_load.wait()
    root[...] = jnp.sqrt(w_ref[...])

    def piece_copy(i, buf, send, recv, device, lo, hi):
        here = piece_rows(i)
        return pltpu.make_async_remote_copy(
            src_ref=code.at[here, lo:hi],
            dst_ref=buf.at[here, lo:hi],
            send_sem=send.at[lax.rem(i + turn, NP)],
            recv_sem=recv.at[lax.rem(i + turn, NP)],
            device_id={"variants": device},
            device_id_type=MESH,
        )

    def down_copy(i, hi):
        return piece_copy(i, ncode, ncode_send, ncode_recv, down, 0, hi)

    def up_copy(i, lo):
        return piece_copy(i, pcode, pcode_send, pcode_recv, up, lo, width)

    def send_far(i):
        @pl.when(send_down_part)
        def _():
            down_copy(i, KL).start()

        @pl.when(send_up_part)
        def _():
            up_copy(i, KL).start()

    def total(x):
        return jnp.sum(x.T, axis=0, keepdims=True)

    def first_pass(k):
        load(k).wait()
        base = lax.rem(k + turn, NP) * SUB

        def sixteen(i):
            here = pl.ds(aligned(base + i * STEP, STEP), STEP)
            zero = jnp.zeros((STEP, LANES), F32)
            w0, w1, w2 = zero, zero, zero
            cnt = jnp.zeros((STEP, LANES), jnp.int32)
            for b in range(blocks):
                lane = slice(b * LANES, (b + 1) * LANES)
                g = gen[here, lane]
                w = jnp.broadcast_to(w_ref[0:1, lane], (STEP, LANES))
                w0 = w0 + jnp.where(g == 0, w, 0.0)
                w1 = w1 + jnp.where(g == 1, w, 0.0)
                w2 = w2 + jnp.where(g == 2, w, 0.0)
                tag = jnp.left_shift(jnp.int32(1), jnp.left_shift(g, 3))
                cnt = cnt + tag
                sacc[:, lane] += tag[:8] + tag[8:]
                code[here, lane] = g.astype(F32).astype(BF16)
            wacc[0, here] = w0
            wacc[1, here] = w1
            wacc[2, here] = w2
            cacc[here] = cnt

        loop(0, SUB // STEP, sixteen)

        @pl.when(lax.rem(k, GROUP) == GROUP - 1)
        def _():
            group = pl.ds(aligned(base + SUB - LANES, LANES), LANES)
            for i in range(3):
                gat[s, i : i + 1, group] = total(wacc[i, group])
            cnt = cacc[group]
            for level in range(4):
                some = jnp.bitwise_and(jnp.right_shift(cnt, 8 * level), 255)
                tally[s, level : level + 1, group] = total(some.astype(F32))

        def send(i):
            @pl.when(send_down_full)
            def _():
                down_copy(i, width).start()

            @pl.when(send_up_full)
            def _():
                up_copy(i, 0).start()

            @pl.when(i < EARLY)
            def _():
                send_far(i)

        @pl.when(k == hold)
        def _():
            pl.semaphore_wait(barrier, greetings)
            loop(0, hold, send)

        @pl.when(k >= hold)
        def _():
            send(k)

    loop(0, NP, first_pass)

    def stat_copy(d, slot):
        return pltpu.make_async_remote_copy(
            src_ref=gat.at[slot],
            dst_ref=gat.at[slot],
            send_sem=stat_send.at[d],
            recv_sem=stat_recv.at[slot],
            device_id={"samples": lax.rem(s + d, S)},
            device_id_type=MESH,
        )

    def tally_copy(d, slot):
        return pltpu.make_async_remote_copy(
            src_ref=tally.at[slot],
            dst_ref=tally.at[slot],
            send_sem=tally_send.at[d],
            recv_sem=tally_recv.at[slot],
            device_id={"samples": lax.rem(s + d, S)},
            device_id_type=MESH,
        )

    loop(1, S, lambda d: stat_copy(d, s).start())
    loop(1, S, lambda d: stat_copy(d, lax.rem(s + d, S)).wait_recv())

    sums = gat[0]
    for t in range(1, S):
        sums = sums + gat[t]
    w0, w1, w2 = sums[0:1], sums[1:2], sums[2:3]
    w_sum = w0 + w1 + w2
    mean = (w1 + 2.0 * w2) / w_sum
    one, two = 1.0 - mean, 2.0 - mean
    ms, os, ts = mean * mean, one * one, two * two
    var = (w0 * ms + w1 * os + w2 * ts) / w_sum
    factor = 1.0 / jnp.sqrt(w_sum * (var + 1e-05))
    par[0:1] = mean
    par[1:2] = factor
    for t in range(S):
        length = jnp.sqrt(gat[t, 0:1] * ms + gat[t, 1:2] * os + gat[t, 2:3] * ts)
        par[2 + t : 3 + t] = jnp.maximum(length * factor, 1e-12)
    spare = par.shape[0] - 2 - S
    if spare:
        par[2 + S :] = jnp.zeros((spare, rows), F32)

    def par_copy(i, dst, device):
        return pltpu.make_async_remote_copy(
            src_ref=par,
            dst_ref=dst,
            send_sem=par_send.at[i],
            recv_sem=par_recv.at[i],
            device_id={"variants": device},
            device_id_type=MESH,
        )

    @pl.when(has_prev)
    def _():
        par_copy(0, npar, down).start()

    @pl.when(from_prev)
    def _():
        par_copy(1, ppar, up).start()

    loop(EARLY, NP, send_far)

    stat_out[...] = jnp.concatenate([mean, var], axis=0)
    loop(1, S, lambda d: tally_copy(d, s).start())

    def start_build(src, col):
        aux[...] = jnp.concatenate([src[0:2], jnp.zeros((6, rows), F32)], axis=0)
        turned = aux[...].T
        for i in range(2):
            col[i] = jnp.broadcast_to(turned[:, i : i + 1], (rows, LANES))

    def build(src, col, lane):
        def of(who):
            line = jnp.zeros((1, rows), F32)
            for t in range(S):
                line = line + src[2 + t : 3 + t] * (who == t).astype(F32)
            return line

        mine, its = of(s), of(mate)
        both = jnp.sqrt(mine * mine + its * its)
        aux[...] = jnp.concatenate(
            [FULL / mine, its, FULL / both, jnp.zeros((5, rows), F32)], axis=0
        )
        turned = aux[...].T
        for i in range(3):
            col[2 + i] = jnp.broadcast_to(turned[:, i : i + 1], (rows, LANES))
        lane[0:1] = 1.0 / mine
        lane[1:2] = its * (1.0 / FULL)
        lane[2:3] = 1.0 / both

    def build_tall(src):
        sizes = []
        for q in range(PAIRS):
            a, b = src[2 + 2 * q : 3 + 2 * q], src[3 + 2 * q : 4 + 2 * q]
            sizes.append(jnp.sqrt(a * a + b * b))
        left = -PAIRS % 8
        if left:
            sizes.append(jnp.zeros((left, rows), F32))
        tall[:, 0 : PAIRS + left] = jnp.concatenate(sizes, axis=0).T

    def scale(src, src_row, dst, dst_row, count, lo, hi, col):
        def sixteen(i):
            here = pl.ds(aligned(src_row + i * STEP, STEP), STEP)
            there = pl.ds(aligned(dst_row + i * STEP, STEP), STEP)
            m, f = col[0, here], col[1, here]
            for b in range(lo // LANES, hi // LANES):
                lane = slice(b * LANES, (b + 1) * LANES)
                d = src[here, lane].astype(F32)
                r = jnp.broadcast_to(root[0:1, lane], (STEP, LANES))
                x = jnp.where(d < 2.5, r * (d - m) * f, 0.0).astype(BF16)
                dst[there, lane] = x

        loop(0, count // STEP, sixteen)

    def rows_of():
        row = lax.rem(s, H) * R
        for q in range(PAIRS):
            spread[q] = jnp.broadcast_to(
                tall[pl.ds(aligned(row, R), R), q : q + 1], (R, LANES)
            )

    start_build(par, col_o)
    scale(code, 0, scaled, 0, rows, 0, width, col_o)
    build(par, col_o, lane_o)

    def dot(a, b):
        return lax.dot_general(
            a, b, (((1,), (1,)), ((), ())), preferred_element_type=F32
        )

    def coded(value, e, line):
        q = jnp.round(value * e * line)
        q = jnp.clip(q, -32767.0, 32767.0)
        return q.astype(jnp.int32).astype(jnp.int16)

    def pack(src, src_row, col, col_row, lane, lane_at, cols, count, dst, dst_row):
        def sixteen(i):
            here = pl.ds(aligned(src_row + i * STEP, STEP), STEP)
            e = col[2, pl.ds(aligned(col_row + i * STEP, STEP), STEP)]
            for b in range(cols // LANES):
                part = slice(b * LANES, (b + 1) * LANES)
                line = lane[0:1, pl.ds(aligned(lane_at + b * LANES, LANES), LANES)]
                dst[pl.ds(aligned(dst_row + i * STEP, STEP), STEP), part] = coded(
                    src[here, part], e, line
                )

        loop(0, count // STEP, sixteen)

    def merge(
        src,
        src_row,
        got,
        got_row,
        col,
        col_row,
        lane,
        lane_at,
        cols,
        count,
        dst,
        dst_row,
        final,
    ):
        def sixteen(i):
            here = pl.ds(aligned(src_row + i * STEP, STEP), STEP)
            line_rows = pl.ds(aligned(col_row + i * STEP, STEP), STEP)
            there = pl.ds(aligned(dst_row + i * STEP, STEP), STEP)
            theirs = pl.ds(aligned(got_row + i * STEP, STEP), STEP)
            d, e = col[3, line_rows], col[4, line_rows]
            for b in range(cols // LANES):
                part = slice(b * LANES, (b + 1) * LANES)
                lanes = pl.ds(aligned(lane_at + b * LANES, LANES), LANES)
                q = got[theirs, part].astype(jnp.int32).astype(F32)
                value = src[here, part] + q * d * lane[1:2, lanes]
                if final:
                    dst[there, part] = value
                else:
                    dst[there, part] = coded(value, e, lane[2:3, lanes])

        loop(0, count // STEP, sixteen)

    def copy_to(src, dst, send, recv, device):
        return pltpu.make_async_remote_copy(
            src_ref=src,
            dst_ref=dst,
            send_sem=send,
            recv_sem=recv,
            device_id=device,
            device_id_type=MESH,
        )

    def yo_copy(j):
        return copy_to(
            ypart_o.at[j], yrcv_o.at[j], yo_send.at[j], yo_recv.at[j], {"samples": mate}
        )

    def zo_copy(j):
        return copy_to(
            zpart_o.at[j],
            zrcv.at[pair],
            zo_send.at[j],
            z_recv.at[pair],
            {"samples": 2 * j + y},
        )

    TALL = min(rows, 256)
    PER = TALL // R

    def own_rows(k):
        first = lax.rem(k * TALL + lax.div(turn * SUB, TALL) * TALL, rows)
        here = pl.ds(aligned(first, TALL), TALL)
        keep_o[here, :] = dot(scaled[here, :], scaled[...])

        def give(i):
            o = lax.div(first, R) + 2 * i + 1 - y
            j = lax.div(o, 2)
            pack(keep_o, o * R, col_o, o * R, lane_o, 0, rows, R, ypart_o.at[j], 0)
            yo_copy(j).start()

        loop(0, PER // 2, give)

    loop(0, rows // TALL, own_rows)

    mate_copy = copy_to(
        smp_mine,
        smp_mate,
        mate_send.at[0],
        mate_recv.at[0],
        {"variants": v + 1 - 2 * (v - 2 * chip)},
    )
    def squares(b):
        lanes = pl.ds(aligned(b * LANES, LANES), LANES)
        sums = [jnp.zeros((8, LANES), F32) for _ in range(4)]
        for i in range(rows // STEP):
            x = scaled[i * STEP : (i + 1) * STEP, lanes].astype(F32)
            x = x * x
            k = 2 * (i % 2)
            sums[k] = sums[k] + x[:8]
            sums[k + 1] = sums[k + 1] + x[8:]
        qacc[:, lanes] = (sums[0] + sums[1]) + (sums[2] + sums[3])

    def sample_sums():
        loop(0, blocks, squares)
        packed = sacc[...]
        tags = [
            jnp.bitwise_and(jnp.right_shift(packed, 8 * level), 255).astype(F32)
            for level in range(3)
        ]
        for q, value in enumerate([tags[0] + tags[1] + tags[2], tags[1], qacc[...]]):
            line = jnp.sum(value, axis=0, keepdims=True)
            for i in range(slabs):
                at = q * slabs + i
                smp_mine[at : at + 1, :] = line[:, i * SLAB : (i + 1) * SLAB]
        mate_copy.start()


    def smp_copy(d, slot):
        return copy_to(
            smp_all.at[slot],
            smp_all.at[slot],
            smp_send.at[d],
            smp_recv.at[slot],
            {"variants": lax.rem(v + 2 * d, V)},
        )

    def share_sums():
        mate_copy.wait_recv()
        smp_all[chip] = smp_mine[...] + smp_mate[...]
        loop(1, C, lambda d: smp_copy(d, chip).start())

    def own_norms():
        for q in range(PAIRS):
            a, b = par[2 + 2 * q : 3 + 2 * q], par[3 + 2 * q : 4 + 2 * q]
            lane_q[q] = jnp.sqrt(a * a + b * b) * (1.0 / FULL)

        @pl.when(s < H)
        def _():
            build_tall(par)
            rows_of()

    def rows_of():
        row = lax.rem(s, H) * R
        for q in range(PAIRS):
            spread[q] = jnp.broadcast_to(
                tall[pl.ds(aligned(row, R), R), q : q + 1], (R, LANES)
            )

    def own_half(i):
        loop(i * (Q // 2), (i + 1) * (Q // 2), collect_own)

    def collect_own(k):
        j = lax.rem(k + lax.div(turn * SUB, TALL) * (PER // 2), Q)
        o = 2 * j + y
        yo_copy(j).wait_recv()
        args = (keep_o, o * R, yrcv_o.at[j], 0, col_o, o * R, lane_o, 0, rows, R)

        @pl.when(o == s)
        def _():
            merge(*args, ld_out, 0, True)

        @pl.when(o != s)
        def _():
            merge(*args, zpart_o.at[j], 0, False)
            zo_copy(j).start()

    def yn_copy(at, size):
        j = lax.div(lax.div(at, R), 2)
        here = pl.ds(aligned(at - lax.div(at, R) * R, size), size)
        unit = lax.div(at, UNIT)
        return copy_to(
            ypart_n.at[j, here],
            yrcv_n.at[j, here],
            yn_send.at[unit],
            yn_recv.at[unit],
            {"samples": mate},
        )

    def zn_copy(at, size):
        r = lax.div(at, R)
        here = pl.ds(aligned(at - r * R, size), size)
        return copy_to(
            zpart_n.at[lax.div(r, 2), here],
            zrcv.at[pair, here],
            zn_send.at[lax.div(at, UNIT)],
            z_recv.at[pair],
            {"samples": H + r},
        )

    def next_rows(k, size):
        return lax.rem(k * size + lax.div(turn * SUB, size) * size, rows)

    def next_parity(at):
        r = lax.div(at, R)
        return r - 2 * lax.div(r, 2) == y

    def collect_next(at, size):
        r = lax.div(at, R)

        @pl.when(next_parity(at))
        def _():
            yn_copy(at, size).wait_recv()
            j = lax.div(r, 2)
            off = at - r * R
            args = (keep_x, at, yrcv_n.at[j], off, col_x, at, lane_o, 0, rows, size)

            @pl.when(H + r == s)
            def _():
                merge(*args, ld_out, off, True)

            @pl.when(H + r != s)
            def _():
                merge(*args, zpart_n.at[j], off, False)
                zn_copy(at, size).start()

    def give_next(at, size):
        r = lax.div(at, R)

        @pl.when(jnp.logical_not(next_parity(at)))
        def _():
            j = lax.div(r, 2)
            pack(
                keep_x, at, col_x, at, lane_o, 0, rows, size, ypart_n.at[j], at - r * R
            )
            yn_copy(at, size).start()

    def next_dot(at, tall_rows, hi):
        def arrived(i):
            down_copy(lax.rem(lax.div(at, SUB) + i + NP - turn, NP), hi).wait_recv()

        loop(0, tall_rows // SUB, arrived)
        scale(ncode, at, other, 0, tall_rows, 0, hi, col_x)
        here = pl.ds(aligned(at, tall_rows), tall_rows)
        keep_x[here, :] = dot(other[0:tall_rows, 0:hi], scaled[:, 0:hi])

    def next_role_full():
        pieces = TALL // R

        def each(at, act):
            loop(0, pieces, lambda i: act(at + i * R, R))

        count = rows // TALL
        for k in range(count):
            at = next_rows(k, TALL)
            next_dot(at, TALL, width)
            each(at, give_next)
            if k == 0:
                own_half(0)
            if k == count - 1:
                own_half(1)
            if k > 0:
                each(next_rows(k - 1, TALL), collect_next)
        sample_sums()
        each(next_rows(count - 1, TALL), collect_next)
        share_sums()
        own_norms()
        next_norms()

    def next_role_part(hi):
        wide = LANES // UNIT
        count = rows // LANES

        def each(at, act):
            loop(0, wide, lambda i: act(at + i * UNIT, UNIT))

        alone = jnp.logical_not(does_full)

        def chunk(k):
            at = next_rows(k, LANES)
            next_dot(at, LANES, hi)
            each(at, give_next)

            @pl.when(jnp.logical_and(k == 0, alone))
            def _():
                own_half(0)

            @pl.when(jnp.logical_and(k == 1, alone))
            def _():
                sample_sums()
                own_half(1)

            @pl.when(k > 0)
            def _():
                each(next_rows(k - 1, LANES), collect_next)

        loop(0, count - 1, chunk)
        next_norms()

        def small(k):
            at = next_rows(count - 1, LANES) + k * UNIT
            next_dot(at, UNIT, hi)
            give_next(at, UNIT)

            @pl.when(k == 0)
            def _():
                each(next_rows(count - 2, LANES), collect_next)

            @pl.when(k > 0)
            def _():
                collect_next(at - UNIT, UNIT)

        loop(0, wide, small)

        @pl.when(alone)
        def _():
            share_sums()
            own_norms()

        collect_next(next_rows(count - 1, LANES) + LANES - UNIT, UNIT)

    def yp_copy(c):
        return copy_to(
            ypart_p.at[c], yrcv_p.at[c], yp_send.at[c], yp_recv.at[c], {"samples": mate}
        )

    def zp_copy(j, c):
        return copy_to(
            zpart_p.at[j, c],
            zrcv_p.at[pair, c],
            zp_send.at[j],
            zp_recv.at[pair],
            {"samples": H + 2 * j + y, "variants": down},
        )

    def collect_prev(c):
        yp_copy(c).wait_recv()

        def one(i):
            j = lax.rem(i + pair, Q)
            o = (2 * j + y) * R
            merge(
                keep_x,
                c * rows + o,
                yrcv_p.at[c, j],
                0,
                col_o,
                o,
                lane_x,
                c * LANES,
                LANES,
                R,
                zpart_p.at[j, c],
                0,
                False,
            )
            zp_copy(j, c).start()

        loop(0, Q, one)

    def prev_dot(c, wide, lo):
        def arrived(i):
            up_copy(lax.rem(c * GROUP + i + NP - turn, NP), lo).wait_recv()

        loop(0, wide * GROUP, arrived)
        scale(pcode, c * LANES, other, 0, wide * LANES, lo, width, col_x)
        got = dot(scaled[:, lo:width], other[0 : wide * LANES, lo:width])
        for i in range(wide):
            here = pl.ds(aligned((c + i) * rows, rows), rows)
            keep_x[here, 0:LANES] = got[:, i * LANES : (i + 1) * LANES]

    def give_prev(c):
        def one(j):
            o = (2 * j + 1 - y) * R
            pack(
                keep_x,
                c * rows + o,
                col_o,
                o,
                lane_x,
                c * LANES,
                LANES,
                R,
                ypart_p.at[c, j],
                0,
            )

        loop(0, Q, one)
        yp_copy(c).start()

    def prev_role(wide, lo, full):
        count = NCP // wide
        first = lax.div(lax.div(turn, GROUP), wide)

        def at(k):
            return lax.rem(k + first, count) * wide

        def each(k, act):
            loop(0, wide, lambda i: act(at(k) + i))

        def chunk(k):
            prev_dot(at(k), wide, lo)
            each(k, give_prev)

        if full:
            chunk(0)
            own_half(0)
            chunk(1)
            own_half(1)
            each(0, collect_prev)
            sample_sums()
        else:
            alone = jnp.logical_not(does_full)
            chunk(0)

            @pl.when(alone)
            def _():
                own_half(0)

            chunk(1)

            @pl.when(alone)
            def _():
                own_half(1)

            each(0, collect_prev)

            @pl.when(alone)
            def _():
                sample_sums()

        def rest(k):
            chunk(k)
            each(k - 1, collect_prev)

        loop(2, count, rest)

        @pl.when(jnp.logical_or(full, jnp.logical_not(does_full)))
        def _():
            share_sums()
            own_norms()

        each(count - 1, collect_prev)

    def with_next():
        par_copy(0, npar, down).wait_recv()
        start_build(npar, col_x)
        build(npar, col_x, lane_x)

    def next_norms():
        @pl.when(s >= H)
        def _():
            build_tall(npar)
            rows_of()


    def with_prev():
        par_copy(1, ppar, up).wait_recv()
        start_build(ppar, col_x)
        build(ppar, col_x, lane_x)


    @pl.when(prev_full)
    def _():
        with_prev()
        prev_role(min(2, NCP), 0, True)

    @pl.when(next_full)
    def _():
        with_next()
        next_role_full()

    @pl.when(prev_part)
    def _():
        with_prev()
        prev_role(1, KL, False)

    @pl.when(next_part)
    def _():
        with_next()
        next_role_part(KL)

    @pl.when(jnp.logical_and(jnp.logical_not(from_next), has_next))
    def _():
        par_copy(0, npar, down).wait_recv()
        next_norms()

    loop(1, S, lambda d: stat_copy(d, s).wait_send())
    loop(1, S, lambda d: tally_copy(d, s).wait_send())
    mate_copy.wait_send()


    @pl.when(has_prev)
    def _():
        par_copy(0, npar, down).wait_send()

    @pl.when(from_prev)
    def _():
        par_copy(1, ppar, up).wait_send()

    @pl.when(send_down_full)
    def _():
        loop(0, NP, lambda i: down_copy(i, width).wait_send())

    @pl.when(send_down_part)
    def _():
        loop(0, NP, lambda i: down_copy(i, KL).wait_send())

    @pl.when(send_up_full)
    def _():
        loop(0, NP, lambda i: up_copy(i, 0).wait_send())

    @pl.when(send_up_part)
    def _():
        loop(0, NP, lambda i: up_copy(i, KL).wait_send())

    loop(1, S, lambda d: tally_copy(d, lax.rem(s + d, S)).wait_recv())
    counts = tally[0]
    for t in range(1, S):
        counts = counts + tally[t]
    count_out[...] = counts.astype(jnp.int32)

    loop(1, C, lambda d: smp_copy(d, lax.rem(chip + d, C)).wait_recv())
    all_sums = smp_all[0]
    for t in range(1, C):
        all_sums = all_sums + smp_all[t]
    call_out[...] = all_sums[: 2 * slabs].astype(jnp.int32)
    share_out[...] = all_sums[2 * slabs :] * F32((width * S) / (rows * V))

    def gather(got, q, part, wide):
        def sixteen(i):
            here = pl.ds(aligned(i * STEP, STEP), STEP)
            e = spread[q, here]
            for b in range(rows // LANES):
                lanes = slice(b * LANES, (b + 1) * LANES)
                line = lane_q[q, 0:1, lanes]
                piece = got[b, here] if wide else got[here, lanes]
                ld_out[here, lanes] += piece.astype(jnp.int32).astype(F32) * e * line

        loop(0, R // STEP, sixteen)

    def gather_pairs(d):
        q = lax.rem(pair + d, PAIRS)
        copy_to(
            zrcv.at[q], zrcv.at[q], zo_send.at[0], z_recv.at[q], {"samples": mate}
        ).wait_recv()
        gather(zrcv.at[q], q, None, False)

    def gather_prev(d):
        q = lax.rem(pair + d, PAIRS)
        copy_to(
            zrcv_p.at[q], zrcv_p.at[q], zp_send.at[0], zp_recv.at[q], {"samples": mate}
        ).wait_recv()
        gather(zrcv_p.at[q], q, None, True)

    @pl.when(s < H)
    def _():
        loop(1, PAIRS, gather_pairs)

    @pl.when(s >= H)
    def _():
        @pl.when(from_next)
        def _():
            loop(1, PAIRS, gather_pairs)

        @pl.when(jnp.logical_not(from_next))
        def _():
            ld_out[...] = jnp.zeros_like(ld_out)

        @pl.when(from_prev)
        def _():
            loop(0, PAIRS, gather_prev)

    def drain_own(j):
        yo_copy(j).wait_send()

        @pl.when(2 * j + y != s)
        def _():
            zo_copy(j).wait_send()

    loop(0, Q, drain_own)

    def drain_next(size):
        def one(k):
            at = k * size
            mine = next_parity(at)

            @pl.when(jnp.logical_not(mine))
            def _():
                yn_copy(at, size).wait_send()

            @pl.when(jnp.logical_and(mine, H + lax.div(at, R) != s))
            def _():
                zn_copy(at, size).wait_send()

        loop(0, rows // size, one)

    @pl.when(next_full)
    def _():
        drain_next(R)

    @pl.when(next_part)
    def _():
        drain_next(UNIT)

    @pl.when(does_prev)
    def _():
        loop(0, NCP, lambda c: yp_copy(c).wait_send())

        def drain(j):
            copy_to(
                zpart_p.at[j], zpart_p.at[j], zp_send.at[j], zp_recv.at[0], {"samples": mate}
            ).wait_send()

        loop(0, Q, drain)

    loop(1, C, lambda d: smp_copy(d, chip).wait_send())


def finish(stats, counts, ld, calls, share, mean, var, counts_o, ld_o, calls_o, share_o):
    slabs = share.shape[0]
    mean[...] = stats[0]
    var[...] = stats[1]
    counts_o[...] = counts[...]
    ld_o[...] = ld[...]
    for i in range(slabs):
        here = slice(i * SLAB, (i + 1) * SLAB)
        for q in range(2):
            calls_o[q : q + 1, here] = calls[q * slabs + i : q * slabs + i + 1]
        share_o[here] = share[i]


def on_device(S, V, genotypes, weights):
    rows, width = genotypes.shape
    R = 2 * rows // S
    H = S // 2
    Q = H // 2
    PAIRS = S // 2
    C = V // 2
    NP = rows // SUB
    NCP = rows // LANES
    units = rows // min(R, 64)
    lines = -(-(2 + S) // 8) * 8
    slabs = width // SLAB
    vmem = pl.BlockSpec(memory_space=pltpu.VMEM)
    dma = pltpu.SemaphoreType.DMA
    results = pl.pallas_call(
        functools.partial(kernel, S, V),
        out_shape=(
            pltpu.VMEM((2, rows), F32),
            pltpu.VMEM((4, rows), jnp.int32),
            pltpu.VMEM((R, rows), F32),
            pltpu.VMEM((2 * slabs, SLAB), jnp.int32),
            pltpu.VMEM((slabs, SLAB), F32),
        ),
        in_specs=[pl.BlockSpec(memory_space=pl.ANY)] * 2,
        out_specs=(vmem,) * 5,
        scratch_shapes=[
            pltpu.VMEM((rows, width), jnp.int32),
            pltpu.VMEM((rows, width), BF16),
            pltpu.VMEM((rows, width), BF16),
            pltpu.VMEM((rows, width), BF16),
            pltpu.VMEM((rows, width), BF16),
            pltpu.VMEM((min(rows, 256), width), BF16),
            pltpu.VMEM((rows, rows), F32),
            pltpu.VMEM((NCP * rows, rows), F32),
            pltpu.VMEM((Q, R, rows), jnp.int16),
            pltpu.VMEM((Q, R, rows), jnp.int16),
            pltpu.VMEM((Q, R, rows), jnp.int16),
            pltpu.VMEM((Q, R, rows), jnp.int16),
            pltpu.VMEM((NCP, Q, R, LANES), jnp.int16),
            pltpu.VMEM((NCP, Q, R, LANES), jnp.int16),
            pltpu.VMEM((Q, R, rows), jnp.int16),
            pltpu.VMEM((Q, R, rows), jnp.int16),
            pltpu.VMEM((Q, NCP, R, LANES), jnp.int16),
            pltpu.VMEM((PAIRS, R, rows), jnp.int16),
            pltpu.VMEM((PAIRS, NCP, R, LANES), jnp.int16),
            pltpu.VMEM((3, rows, LANES), F32),
            pltpu.VMEM((rows, LANES), jnp.int32),
            pltpu.VMEM((8, width), jnp.int32),
            pltpu.VMEM((8, width), F32),
            pltpu.VMEM((1, width), F32),
            pltpu.VMEM((S, 3, rows), F32),
            pltpu.VMEM((S, 4, rows), F32),
            pltpu.VMEM((lines, rows), F32),
            pltpu.VMEM((lines, rows), F32),
            pltpu.VMEM((lines, rows), F32),
            pltpu.VMEM((8, rows), F32),
            pltpu.VMEM((5, rows, LANES), F32),
            pltpu.VMEM((5, rows, LANES), F32),
            pltpu.VMEM((8, rows), F32),
            pltpu.VMEM((8, rows), F32),
            pltpu.VMEM((PAIRS, 1, rows), F32),
            pltpu.VMEM((rows, LANES), F32),
            pltpu.VMEM((PAIRS, R, LANES), F32),
            pltpu.VMEM((3 * slabs, SLAB), F32),
            pltpu.VMEM((3 * slabs, SLAB), F32),
            pltpu.VMEM((C, 3 * slabs, SLAB), F32),
            pltpu.VMEM((1, width), F32),
            dma((NP,)),
            dma(()),
            dma((NP,)),
            dma((NP,)),
            dma((NP,)),
            dma((NP,)),
            dma((S,)),
            dma((S,)),
            dma((S,)),
            dma((S,)),
            dma((2,)),
            dma((2,)),
            dma((Q,)),
            dma((Q,)),
            dma((units,)),
            dma((units,)),
            dma((NCP,)),
            dma((NCP,)),
            dma((Q,)),
            dma((units,)),
            dma((Q,)),
            dma((PAIRS,)),
            dma((PAIRS,)),
            dma((1,)),
            dma((1,)),
            dma((C,)),
            dma((C,)),
        ],
        compiler_params=pltpu.CompilerParams(
            collective_id=0, has_side_effects=True, vmem_limit_bytes=60 * 1024 * 1024
        ),
        name="window_stats",
    )(genotypes, weights.reshape(1, width))
    results = [pltpu.with_memory_space_constraint(x, pltpu.VMEM) for x in results]
    return pl.pallas_call(
        finish,
        out_shape=(
            jax.ShapeDtypeStruct((rows,), F32),
            jax.ShapeDtypeStruct((rows,), F32),
            jax.ShapeDtypeStruct((4, rows), jnp.int32),
            jax.ShapeDtypeStruct((R, rows), F32),
            jax.ShapeDtypeStruct((2, width), jnp.int32),
            jax.ShapeDtypeStruct((width,), F32),
        ),
        in_specs=[vmem] * 5,
        out_specs=(vmem,) * 6,
        name="finish",
    )(*results)


def solution(mesh):
    body = functools.partial(on_device, mesh.shape["samples"], mesh.shape["variants"])
    return jax.shard_map(
        body,
        mesh=mesh,
        in_specs=(P("variants", "samples"), P("samples")),
        out_specs=(
            P("variants"),
            P("variants"),
            P(None, "variants"),
            P("samples", "variants"),
            P(None, "samples"),
            P("samples"),
        ),
        check_vma=False,
    )
```
